256 devices in a mesh: inst: 4 (over z_hi), shard: 64 (over y, x, z_lo, core).
Axes of the slice: x: 4, y: 4, z: 8 (z_hi: 4, z_lo: 2; z = z_hi * 2 + z_lo), core: 2. Of those that a mesh axis runs over, the one named last changes fastest.
Arguments:
- master_old: float32 [4, 128, 65536], P('inst', 'shard'), may hold values from -3 to 3
- first_old: float32 [4, 128, 65536], P('inst', 'shard'), may hold values from -2 to 2
- second_old: float32 [4, 128, 65536], P('inst', 'shard'), may hold values from 0.01 to 1
- healthy: int32 [64], replicated, may hold values from 0 to 3
- slice_table: int32 [128], replicated, may hold values from 0 to 127, as said below
Outputs:
- master_new: float32 [4, 128, 65536], P('inst', 'shard')
- first_new: float32 [4, 128, 65536], P('inst', 'shard')
- second_new: float32 [4, 128, 65536], P('inst', 'shard')
- params_half: bfloat16 [4, 128, 65536], P('inst', 'shard')
- checksum: float32 [4, 2], P('inst')
The draws below stay inside these ranges and needn't reach their ends.
Inputs may be any that keep to these rules, and one draw needn't show every extreme that they name: slice_table[k] = (k + slice_table[0]) mod 128 for every k, with slice_table[0] odd and at least 3.
All inputs are finite; a program needn't handle non-finite values.
Results may differ from the reference program's by a relative error of at most 0.001.
Values sent between devices are 32-bit elements; how exact they have to be, the bound alone decides.
A program may use at most 64 MiB of HBM per device.

```python
import math
import jax
import jax.numpy as jnp

SLICE = 65536
OLD = 128
N_INST = 4
N_SHARD = 64


def draw_slice_table(key, part):
    rotation = 2 * jax.random.randint(jax.random.fold_in(key, 11), (), 1, OLD // 2) + 1
    return ((jnp.arange(OLD, dtype=jnp.int32) + rotation) % OLD).astype(jnp.int32)


def with_ends(array, key, least, high):
    shape = array.shape
    spot = [jax.random.randint(jax.random.fold_in(key, axis), (), 0, shape[axis]) for axis in range(len(shape))]
    array = array.at[tuple(spot)].set(least)
    longest = shape.index(max(shape))
    spot[longest] = (spot[longest] + 1) % shape[longest]
    return array.at[tuple(spot)].set(high)


def block_scale(stream_key, shape, pieces, least, largest):
    def one(dim, parts):
        heights = jax.random.uniform(jax.random.fold_in(jax.random.fold_in(stream_key, 6), dim), (parts,), jnp.float32, least / len(pieces), largest / len(pieces))
        return jnp.repeat(jnp.exp(heights), shape[dim] // parts).reshape((-1,) + (1,) * (len(shape) - dim - 1))

    gain = one(*pieces[0])
    for cut in pieces[1:]:
        gain = gain * one(*cut)
    return gain


def centred(key, extent, width, reach, shards=(), kind=jnp.bfloat16):
    drawn = width * jax.random.normal(key, extent, jnp.float32)
    if shards:
        drawn = drawn * block_scale(key, extent, shards, -0.22, 0.18)
    return jnp.clip(drawn, -reach, reach).astype(kind)


def setup_inputs(seed: int = 0) -> dict:
    key_of = jax.random.split(jax.random.key(seed), 6)
    return {
        "master_old": centred(key_of[0], (N_INST, OLD, SLICE), 0.5, 3.0, ((0, 4), (1, 64)), jnp.float32),
        "first_old": centred(key_of[1], (N_INST, OLD, SLICE), 0.3, 2.0, ((0, 4), (1, 64)), jnp.float32),
        "second_old": jnp.clip(jnp.exp(math.log(1.0) - 4.6051702 * jax.random.uniform(key_of[2], (N_INST, OLD, SLICE), jnp.float32) ** block_scale(key_of[2], (N_INST, OLD, SLICE), ((0, 4), (1, 64)), -0.2, 0.2)), 0.01, 1.0),
        "healthy": with_ends(jax.random.randint(key_of[3], (N_SHARD,), 0, N_INST), jax.random.fold_in(key_of[3], 1), 0, N_INST - 1).astype(jnp.int32),
        "slice_table": draw_slice_table(jax.random.fold_in(key_of[5], 71), 0),
    }


def position_keys(flat_rows, columns):
    residue = (flat_rows.astype(jnp.int32) * (columns % 101)) % 101
    offsets = jnp.arange(columns, dtype=jnp.int32)
    cycled = (residue[:, None] + offsets[None, :]) % 101
    return ((cycled * 37) % 101 + 1).astype(jnp.float32) / 101.0


def reference(master_old, first_old, second_old, healthy, slice_table):
    inverse = jnp.zeros((OLD,), jnp.int32).at[slice_table].set(jnp.arange(OLD, dtype=jnp.int32))
    row_source = jnp.repeat(healthy.astype(jnp.int32), 2)
    row_index = jnp.arange(OLD, dtype=jnp.int32)

    def select_rows(stacked):
        source = stacked[row_source, row_index]
        return jnp.take(source, inverse, axis=0)

    master = select_rows(master_old)
    first_moment = select_rows(first_old)
    second = select_rows(second_old)
    combined = master + first_moment + second
    weights = position_keys(jnp.arange(OLD, dtype=jnp.int32), SLICE)
    scale = jnp.float32(2 * SLICE)
    total_all = jnp.sum(combined * weights) / scale
    total_master = jnp.sum(master * weights) / scale
    sums = jnp.stack([total_all, total_master]).astype(jnp.float32)

    def replicate(stacked):
        return jnp.broadcast_to(stacked[None], (N_INST,) + stacked.shape)

    return (replicate(master), replicate(first_moment), replicate(second),
            replicate(master.astype(jnp.bfloat16)), replicate(sums))
```

```python
import functools

import jax
import jax.numpy as jnp
from jax import lax
from jax.experimental import pallas as pl
from jax.experimental.pallas import tpu as pltpu
from jax.sharding import PartitionSpec as P

MESH = pl.DeviceIdType.MESH
KINDS = 3
GROUP = 16


def to_lines(shard, pieces):
    rows, columns = shard.shape[1:]
    lanes = shard.reshape(rows, columns // 128, 128)
    return lanes.transpose(1, 0, 2).reshape(pieces, columns * rows // (128 * pieces), 128)


def from_lines(lines, rows, columns):
    lanes = lines.reshape(columns // 128, rows, 128)
    return lanes.transpose(1, 0, 2).reshape(1, rows, columns)


def kernel(n_inst, n_shard, healthy, table, master, first, second, out, sums_out,
           own, got, staged, final, part, part_got, total, total_got,
           load_sem, spread_send, spread_recv, deal_send, deal_recv,
           part_send, part_recv, total_send, total_recv, store_sem):
    n_all = n_inst * n_shard
    inst = lax.axis_index("inst")
    shard = lax.axis_index("shard")
    me = inst * n_shard + shard
    height = own.shape[2]

    loads = [
        pltpu.make_async_copy(source, own.at[:, kind], load_sem.at[kind])
        for kind, source in enumerate((master, first, second))
    ]
    for load in loads:
        load.start()
    for load in loads:
        load.wait()

    def peer(step):
        to_inst = lax.rem(inst + lax.rem(step, n_inst), n_inst)
        to_shard = lax.rem(shard + step // n_inst, n_shard)
        return to_inst, to_shard

    def spread(step, carry):
        to_inst, to_shard = peer(step)
        pltpu.make_async_remote_copy(
            src_ref=own.at[to_inst * n_shard + to_shard],
            dst_ref=got.at[me],
            send_sem=spread_send,
            recv_sem=spread_recv,
            device_id=(to_inst, to_shard),
            device_id_type=MESH,
        ).start()
        return carry

    lax.fori_loop(1, n_all, spread, 0)
    got[me] = own[me]

    block = 16
    shape = (block, height, 128)
    line = lax.broadcasted_iota(jnp.int32, shape, 1)
    lane = lax.broadcasted_iota(jnp.int32, shape, 2)
    piece = lax.broadcasted_iota(jnp.int32, shape, 0)
    row = line & 1
    slice_0, slice_1 = table[2 * shard], table[2 * shard + 1]
    row_base = jnp.where(row == 0, slice_0 * 88, slice_1 * 88)
    base = row_base + piece * (64 * height) + (line >> 1) * 128 + lane

    def mod_101(x):
        return x - ((x * 10382) >> 20) * 101

    def weigh(step, carry):
        all_sum, master_sum = carry
        at = pl.ds(step * block, block)
        key = mod_101(mod_101(base + step * (block * 64 * height)) * 37) + 1
        key = key.astype(jnp.float32)
        m = own[at, 0]
        term = m * key
        rest = (own[at, 1] + own[at, 2]) * key
        return all_sum + (term + rest), master_sum + term

    zero = jnp.zeros(shape, jnp.float32)
    all_sum, master_sum = lax.fori_loop(0, n_all // block, weigh, (zero, zero))
    mine = healthy[shard] == inst
    both = jnp.stack([all_sum.sum(axis=0).sum(axis=0), master_sum.sum(axis=0).sum(axis=0)])
    part[...] = jnp.where(mine, both, 0.0)

    per_y = n_shard // 4
    y, low = shard // per_y, lax.rem(shard, per_y)
    group_at = inst * 4 + y

    def share_part(step, carry):
        to = lax.rem(group_at + step, GROUP)
        pltpu.make_async_remote_copy(
            src_ref=part,
            dst_ref=part_got.at[group_at],
            send_sem=part_send,
            recv_sem=part_recv,
            device_id=(to // 4, lax.rem(to, 4) * per_y + low),
            device_id_type=MESH,
        ).start()
        return carry

    lax.fori_loop(1, GROUP, share_part, 0)
    part_got[group_at] = part[...]

    def wait_for(source, target, send_sem, recv_sem):
        return pltpu.make_async_remote_copy(
            src_ref=source,
            dst_ref=target,
            send_sem=send_sem,
            recv_sem=recv_sem,
            device_id=(inst, shard),
            device_id_type=MESH,
        )

    most = pl.ds(0, n_all - 1)
    spread_all = wait_for(own.at[most], got.at[most], spread_send, spread_recv)
    spread_all.wait_recv()

    rotation = table[0] >> 1

    def stage(new, carry):
        low_from = (new - rotation - 1) & (n_shard - 1)
        high_from = (new - rotation) & (n_shard - 1)
        low = got[healthy[low_from] * n_shard + low_from]
        high = got[healthy[high_from] * n_shard + high_from]
        lines = []
        for pair in range(0, height, 2):
            lines += [low[:, pair + 1:pair + 2], high[:, pair:pair + 1]]
        staged[new] = jnp.concatenate(lines, axis=1)
        return carry

    lax.fori_loop(0, n_shard, stage, 0)

    def deal(step, carry):
        to_inst, to_shard = peer(step)
        pltpu.make_async_remote_copy(
            src_ref=staged.at[to_shard],
            dst_ref=final.at[:, me],
            send_sem=deal_send,
            recv_sem=deal_recv,
            device_id=(to_inst, to_shard),
            device_id_type=MESH,
        ).start()
        return carry

    lax.fori_loop(1, n_all, deal, 0)
    final[:, me] = staged[shard]

    few = pl.ds(0, GROUP - 1)
    parts_all = wait_for(part_got.at[few], part_got.at[few], part_send, part_recv)
    parts_all.wait_recv()
    total[...] = part_got[...].sum(axis=0)

    def share_total(step, carry):
        to = lax.rem(low + step, GROUP)
        pltpu.make_async_remote_copy(
            src_ref=total,
            dst_ref=total_got.at[low],
            send_sem=total_send,
            recv_sem=total_recv,
            device_id=(inst, y * per_y + to),
            device_id_type=MESH,
        ).start()
        return carry

    lax.fori_loop(1, GROUP, share_total, 0)
    total_got[low] = total[...]
    totals_all = wait_for(total_got.at[few], total_got.at[few], total_send, total_recv)
    totals_all.wait_recv()
    sums_out[...] = total_got[...].sum(axis=0)

    deal_all = wait_for(own.at[most], final.at[:, most], deal_send, deal_recv)
    deal_all.wait_recv()
    store = pltpu.make_async_copy(final, out, store_sem)
    store.start()
    spread_all.wait_send()
    parts_all.wait_send()
    totals_all.wait_send()
    deal_all.wait_send()
    store.wait()


def on_device(n_inst, n_shard, master_old, first_old, second_old, healthy, slice_table):
    rows, columns = master_old.shape[1:]
    n_all = n_inst * n_shard
    height = rows * columns // (128 * n_all)
    lines = [to_lines(a, n_all) for a in (master_old, first_old, second_old)]
    anywhere = pl.BlockSpec(memory_space=pl.ANY)
    vmem = pl.BlockSpec(memory_space=pltpu.VMEM)
    smem = pl.BlockSpec(memory_space=pltpu.SMEM)
    dma = pltpu.SemaphoreType.DMA
    out, sums = pl.pallas_call(
        functools.partial(kernel, n_inst, n_shard),
        out_shape=(
            jax.ShapeDtypeStruct((KINDS, n_all, height, 128), jnp.float32),
            jax.ShapeDtypeStruct((2, 128), jnp.float32),
        ),
        in_specs=[smem, smem, anywhere, anywhere, anywhere],
        out_specs=(anywhere, vmem),
        scratch_shapes=[
            pltpu.VMEM((n_all, KINDS, height, 128), jnp.float32),
            pltpu.VMEM((n_all, KINDS, height, 128), jnp.float32),
            pltpu.VMEM((n_shard, KINDS, height, 128), jnp.float32),
            pltpu.VMEM((KINDS, n_all, height, 128), jnp.float32),
            pltpu.VMEM((2, 128), jnp.float32),
            pltpu.VMEM((GROUP, 2, 128), jnp.float32),
            pltpu.VMEM((2, 128), jnp.float32),
            pltpu.VMEM((GROUP, 2, 128), jnp.float32),
            dma((KINDS,)),
            dma, dma, dma, dma, dma, dma, dma, dma, dma,
        ],
        compiler_params=pltpu.CompilerParams(has_side_effects=True),
    )(healthy, slice_table, *lines)
    master, first_moment, second = (from_lines(out[k], rows, columns) for k in range(KINDS))
    checksum = jnp.sum(sums, axis=1).reshape(1, 2) * (1.0 / (101.0 * 2.0 * columns))
    return master, first_moment, second, master.astype(jnp.bfloat16), checksum


def solution(mesh):
    per_slice = P("inst", "shard", None)
    return jax.shard_map(
        functools.partial(on_device, mesh.shape["inst"], mesh.shape["shard"]),
        mesh=mesh,
        in_specs=(per_slice, per_slice, per_slice, P(), P()),
        out_specs=(per_slice, per_slice, per_slice, per_slice, P("inst", None)),
        check_vma=False,
    )
```

```python
import functools

import jax
import jax.numpy as jnp
from jax import lax
from jax.experimental import pallas as pl
from jax.experimental.pallas import tpu as pltpu
from jax.sharding import PartitionSpec as P

MESH = pl.DeviceIdType.MESH
KINDS = 3
CHUNKS = 2
SIDE = 8


def to_pieces(shard, pieces):
    rows, columns = shard.shape[1:]
    lines = shard.reshape(rows, columns // 128, 128).transpose(1, 0, 2)
    return lines.reshape(*pieces, rows * columns // (128 * CHUNKS * pieces[1] * pieces[2] * 2), 128)


def from_pieces(pieces, rows, columns):
    lines = pieces.reshape(columns // 128, rows, 128)
    return lines.transpose(1, 0, 2).reshape(1, rows, columns)


def mod_101(x):
    return x - ((x * 10382) >> 20) * 101


def kernel(n_inst, n_shard, healthy, table, master, first, second, out, sums_out,
           own, relayed, mixed, staged, final, part, part_got, row, row_got, total, total_got,
           load_sem, relay_send, relay_recv, spread_send, spread_recv,
           deal_send, deal_recv, near_recv, far_send, far_recv,
           part_send, part_recv, row_send, row_recv, total_send, total_recv, store_sem, *got):
    inst = lax.axis_index("inst")
    shard = lax.axis_index("shard")
    pairs = n_shard // 2
    pair, core = shard // 2, lax.rem(shard, 2)
    height = own.shape[5]
    after = lax.rem(inst + 1, n_inst)
    across = lax.rem(inst + 2, n_inst)
    before = lax.rem(inst + 3, n_inst)

    def copy(source, target, send_sem, recv_sem, to_inst, to_shard):
        return pltpu.make_async_remote_copy(
            src_ref=source,
            dst_ref=target,
            send_sem=send_sem,
            recv_sem=recv_sem,
            device_id=(to_inst, to_shard),
            device_id_type=MESH,
        )

    def waiting(target, send_sem, recv_sem):
        return copy(target, target, send_sem, recv_sem, inst, shard)

    loads = [
        pltpu.make_async_copy(source, own.at[:, :, :, :, kind], load_sem.at[kind])
        for kind, source in enumerate((master, first, second))
    ]
    for load in loads:
        load.start()

    barrier = pltpu.get_barrier_semaphore()

    def greet(step, carry):
        to_shard = lax.rem(shard + step, n_shard)
        for to_inst in (after, before, inst):
            pl.semaphore_signal(barrier, inc=1, device_id=(to_inst, to_shard), device_id_type=MESH)
        return carry

    for to_inst in (after, across, before):
        pl.semaphore_signal(barrier, inc=1, device_id=(to_inst, shard), device_id_type=MESH)
    lax.fori_loop(1, n_shard, greet, 0)

    for load in loads:
        load.wait()

    block = (1, 1, 8, 2)
    shape = (*block, height, 128)
    at_pair = lax.broadcasted_iota(jnp.int32, shape, 2)
    at_core = lax.broadcasted_iota(jnp.int32, shape, 3)
    line = lax.broadcasted_iota(jnp.int32, shape, 4)
    lane = lax.broadcasted_iota(jnp.int32, shape, 5)
    slice_0, slice_1 = table[2 * shard], table[2 * shard + 1]
    row_base = jnp.where((line & 1) == 0, slice_0 * 88, slice_1 * 88)
    width = 64 * height
    base = row_base + (at_pair * 2 + at_core) * width + (line >> 1) * 128 + lane
    blocks = pairs // 8

    def weigh(step, carry):
        all_sum, master_sum = carry
        chunk = step // (n_inst * blocks)
        of_inst = lax.rem(step // blocks, n_inst)
        at = (pl.ds(chunk, 1), pl.ds(of_inst, 1), pl.ds(lax.rem(step, blocks) * 8, 8))
        key = mod_101(mod_101(base + step * (16 * width)) * 37) + 1
        key = key.astype(jnp.float32)
        m = own[at[0], at[1], at[2], :, 0]
        term = m * key
        rest = (own[at[0], at[1], at[2], :, 1] + own[at[0], at[1], at[2], :, 2]) * key
        return all_sum + (term + rest), master_sum + term

    zero = jnp.zeros(shape, jnp.float32)
    sums = lax.fori_loop(0, CHUNKS * n_inst * blocks, weigh, (zero, zero))
    mine = healthy[shard] == inst
    both = jnp.stack([s.reshape(16 * height, 128).sum(axis=0) for s in sums])
    part[...] = jnp.where(mine, both, 0.0)

    pl.semaphore_wait(barrier, 3 * n_shard)

    for to_inst in (after, across, before):
        copy(part, part_got.at[inst], part_send, part_recv, to_inst, shard).start()
    part_got[inst] = part[...]

    sides = ((after, 0), (before, 1))
    for chunk in range(CHUNKS):
        for to_inst, side in sides:
            copy(
                own.at[chunk, across, :, side], relayed.at[chunk, side],
                relay_send.at[chunk, side], relay_recv.at[chunk, side], to_inst, shard,
            ).start()

    def spread_to(chunk, source, slot, to_inst, to_shard):
        copy(
            source, got[chunk].at[slot * n_shard + shard],
            spread_send.at[chunk], spread_recv.at[chunk], to_inst, to_shard,
        ).start()

    def spread_own(chunk):
        partner = 1 - core
        spread_to(chunk, own.at[chunk, inst, pair, partner], 0, inst, pair * 2 + partner)
        got[chunk][shard] = own[chunk, inst, pair, core]

        def spread(step, carry):
            to = lax.rem(pair + step, pairs)
            spread_to(chunk, own.at[chunk, after, to, 1], 1, after, to * 2 + 1)
            spread_to(chunk, own.at[chunk, before, to, 0], 2, before, to * 2)

            @pl.when(step > 0)
            def _():
                spread_to(chunk, own.at[chunk, inst, to, 0], 0, inst, to * 2)
                spread_to(chunk, own.at[chunk, inst, to, 1], 0, inst, to * 2 + 1)

            return carry

        lax.fori_loop(0, pairs, spread, 0)

    def spread_mixed(chunk):
        of_mine = healthy[shard]
        for (to_inst, side), from_inst in zip(sides, (before, after)):
            waiting(relayed.at[chunk, side], relay_send.at[chunk, side], relay_recv.at[chunk, side]).wait_recv()

            def mix(step, carry):
                at = pl.ds(step * 4, 4)
                mixed[chunk, side, at] = jnp.where(
                    of_mine == from_inst, relayed[chunk, side, at], own[chunk, to_inst, at, side]
                )
                return carry

            lax.fori_loop(0, pairs // 4, mix, 0)

        def spread(step, carry):
            to = lax.rem(pair + step, pairs)
            spread_to(chunk, mixed.at[chunk, 0, to], 1, after, to * 2)
            spread_to(chunk, mixed.at[chunk, 1, to], 2, before, to * 2 + 1)
            return carry

        lax.fori_loop(0, pairs, spread, 0)

    for chunk in range(CHUNKS):
        spread_own(chunk)

    some = pl.ds(0, n_inst - 1)
    waiting(part_got.at[some], part_send, part_recv).wait()
    row[...] = part_got[...].sum(axis=0)
    side_at, place = shard // SIDE, lax.rem(shard, SIDE)

    def share_row(step, carry):
        to = lax.rem(place + step, SIDE)
        copy(row, row_got.at[place], row_send, row_recv, inst, side_at * SIDE + to).start()
        return carry

    lax.fori_loop(1, SIDE, share_row, 0)
    row_got[place] = row[...]

    for chunk in range(CHUNKS):
        spread_mixed(chunk)

    rotation = table[0] >> 1
    nearly = pl.ds(0, 3 * n_shard - 1)

    def held(chunk, owner):
        turn = (healthy[owner] - inst) & 3
        slot = jnp.where(turn == 0, 0, jnp.where(turn == 3, 1, jnp.where(turn == 1, 2, 1 + core)))
        return got[chunk][slot * n_shard + owner]

    def deal(chunk):
        waiting(got[chunk].at[nearly], spread_send.at[chunk], spread_recv.at[chunk]).wait_recv()

        def stage(new, carry):
            low = held(chunk, (new - rotation - 1) & (n_shard - 1))
            high = held(chunk, (new - rotation) & (n_shard - 1))
            lines = []
            for at in range(0, height, 2):
                lines += [low[:, at + 1:at + 2], high[:, at:at + 1]]
            staged[chunk, new] = jnp.concatenate(lines, axis=1)
            return carry

        lax.fori_loop(0, n_shard, stage, 0)
        near = lax.rem(inst + 3 + 2 * core, n_inst)
        other = lax.rem(inst + 1 + 2 * core, n_inst)
        place_there = final.at[:, chunk, inst, pair, core]

        def deal_near(step, carry):
            to = lax.rem(shard + step, n_shard)
            copy(staged.at[chunk, to], place_there, deal_send.at[chunk], near_recv.at[chunk, core], near, to).start()
            return carry

        def deal_rest(step, carry):
            to = lax.rem(shard + step, n_shard)
            copy(staged.at[chunk, to], place_there, deal_send.at[chunk], deal_recv.at[chunk], other, to).start()

            @pl.when(step > 0)
            def _():
                copy(staged.at[chunk, to], place_there, deal_send.at[chunk], deal_recv.at[chunk], inst, to).start()

            return carry

        lax.fori_loop(0, n_shard, deal_near, 0)
        lax.fori_loop(0, n_shard, deal_rest, 0)
        final[:, chunk, inst, pair, core] = staged[chunk, shard]

    def pass_on(chunk):
        for side, from_inst, to_inst in ((0, after, before), (1, before, after)):
            there = final.at[:, chunk, from_inst, :, side]
            waiting(there, deal_send.at[chunk], near_recv.at[chunk, side]).wait_recv()
            copy(there, there, far_send.at[chunk, side], far_recv.at[chunk, side], to_inst, shard).start()

    for chunk in range(CHUNKS):
        deal(chunk)
        if chunk == 0:
            few = pl.ds(0, SIDE - 1)
            waiting(row_got.at[few], row_send, row_recv).wait()
            total[...] = row_got[...].sum(axis=0)

            def share_total(step, carry):
                to = lax.rem(side_at + step, SIDE)
                copy(total, total_got.at[side_at], total_send, total_recv, inst, to * SIDE + place).start()
                return carry

            lax.fori_loop(1, SIDE, share_total, 0)
            total_got[side_at] = total[...]
    for chunk in range(CHUNKS):
        pass_on(chunk)

    waiting(total_got.at[pl.ds(0, SIDE - 1)], total_send, total_recv).wait()
    sums_out[...] = total_got[...].sum(axis=0)

    rest = pl.ds(0, 2 * n_shard - 1)
    for chunk in range(CHUNKS):
        waiting(got[chunk].at[rest], deal_send.at[chunk], deal_recv.at[chunk]).wait_recv()
        for side in range(2):
            waiting(
                final.at[:, chunk, across, :, side], far_send.at[chunk, side], far_recv.at[chunk, side]
            ).wait_recv()
        pltpu.make_async_copy(final.at[:, chunk], out.at[:, chunk], store_sem.at[chunk]).start()
    for chunk in range(CHUNKS):
        waiting(got[chunk].at[nearly], spread_send.at[chunk], spread_recv.at[chunk]).wait_send()
        waiting(got[chunk].at[nearly], deal_send.at[chunk], deal_recv.at[chunk]).wait_send()
        for side in range(2):
            waiting(relayed.at[chunk, side], relay_send.at[chunk, side], relay_recv.at[chunk, side]).wait_send()
            waiting(
                final.at[:, chunk, across, :, side], far_send.at[chunk, side], far_recv.at[chunk, side]
            ).wait_send()
        pltpu.make_async_copy(final.at[:, chunk], out.at[:, chunk], store_sem.at[chunk]).wait()


def on_device(n_inst, n_shard, master_old, first_old, second_old, healthy, slice_table):
    rows, columns = master_old.shape[1:]
    pairs = n_shard // 2
    pieces = (CHUNKS, n_inst, pairs, 2)
    arrays = [to_pieces(a, pieces) for a in (master_old, first_old, second_old)]
    tile = arrays[0].shape[4:]
    anywhere = pl.BlockSpec(memory_space=pl.ANY)
    vmem = pl.BlockSpec(memory_space=pltpu.VMEM)
    smem = pl.BlockSpec(memory_space=pltpu.SMEM)
    dma = pltpu.SemaphoreType.DMA

    def buffer(*shape):
        return pltpu.VMEM((*shape, *tile), jnp.float32)

    def sums(*shape):
        return pltpu.VMEM((*shape, 2, 128), jnp.float32)

    out, checks = pl.pallas_call(
        functools.partial(kernel, n_inst, n_shard),
        out_shape=(
            jax.ShapeDtypeStruct((KINDS, *pieces, *tile), jnp.float32),
            jax.ShapeDtypeStruct((2, 128), jnp.float32),
        ),
        in_specs=[smem, smem, anywhere, anywhere, anywhere],
        out_specs=(anywhere, vmem),
        scratch_shapes=[
            buffer(*pieces, KINDS),
            buffer(CHUNKS, 2, pairs, KINDS),
            buffer(CHUNKS, 2, pairs, KINDS),
            buffer(CHUNKS, n_shard, KINDS),
            buffer(KINDS, *pieces),
            sums(), sums(n_inst), sums(), sums(SIDE), sums(), sums(SIDE),
            dma((KINDS,)),
            dma((CHUNKS, 2)), dma((CHUNKS, 2)),
            dma((CHUNKS,)), dma((CHUNKS,)),
            dma((CHUNKS,)), dma((CHUNKS,)), dma((CHUNKS, 2)),
            dma((CHUNKS, 2)), dma((CHUNKS, 2)),
            dma, dma, dma, dma, dma, dma,
            dma((CHUNKS,)),
            *[buffer(3 * n_shard, KINDS) for _ in range(CHUNKS)],
        ],
        compiler_params=pltpu.CompilerParams(collective_id=0, has_side_effects=True),
    )(healthy, slice_table, *arrays)
    master, first_moment, second = (from_pieces(out[k], rows, columns) for k in range(KINDS))
    checksum = jnp.sum(checks, axis=1).reshape(1, 2) * (1.0 / (101.0 * 2.0 * columns))
    return master, first_moment, second, master.astype(jnp.bfloat16), checksum


def solution(mesh):
    per_slice = P("inst", "shard", None)
    return jax.shard_map(
        functools.partial(on_device, mesh.shape["inst"], mesh.shape["shard"]),
        mesh=mesh,
        in_specs=(per_slice, per_slice, per_slice, P(), P()),
        out_specs=(per_slice, per_slice, per_slice, per_slice, P("inst", None)),
        check_vma=False,
    )
```

```python
import functools
import math

import jax
import jax.numpy as jnp
from jax import lax
from jax.experimental import pallas as pl
from jax.experimental.pallas import tpu as pltpu
from jax.sharding import PartitionSpec as P

MESH = pl.DeviceIdType.MESH
KINDS = 3
CHUNKS = 2
SIDE = 8


def to_pieces(shard, pieces):
    rows, columns = shard.shape[1:]
    lines = shard.reshape(rows, columns // 128, 128).transpose(1, 0, 2)
    return lines.reshape(*pieces, rows * columns // (128 * math.prod(pieces)), 128)


def from_pieces(pieces, rows, columns):
    lines = pieces.reshape(columns // 128, rows, 128)
    return lines.transpose(1, 0, 2).reshape(1, rows, columns)


def mod_101(x):
    return x - ((x * 10382) >> 20) * 101


def kernel(n_inst, n_shard, healthy, table, master, first, second, out, sums_out,
           own, cross_in, cross_out, level_in, level_out, staged, final,
           part, part_got, row, row_got, total, total_got,
           load_sem, relay_send, relay_recv, spread_send, spread_recv,
           deal_send, deal_recv, pass_recv, far_send, far_recv,
           part_send, part_recv, row_send, row_recv, total_send, total_recv, store_sem, *got):
    inst = lax.axis_index("inst")
    shard = lax.axis_index("shard")
    spots = n_shard // 4
    spot, level, core = shard // 4, lax.rem(shard // 2, 2), lax.rem(shard, 2)
    flip = 1 - level
    height = own.shape[6]
    after = lax.rem(inst + 1, n_inst)
    across = lax.rem(inst + 2, n_inst)
    before = lax.rem(inst + 3, n_inst)
    near = lax.rem(inst + 3 + 2 * level, n_inst)
    far = lax.rem(inst + 1 + 2 * level, n_inst)

    def copy(source, target, send_sem, recv_sem, to_inst, to_shard):
        return pltpu.make_async_remote_copy(
            src_ref=source,
            dst_ref=target,
            send_sem=send_sem,
            recv_sem=recv_sem,
            device_id=(to_inst, to_shard),
            device_id_type=MESH,
        )

    def waiting(target, send_sem, recv_sem):
        return copy(target, target, send_sem, recv_sem, inst, shard)

    loads = [
        pltpu.make_async_copy(source, own.at[:, :, :, :, :, kind], load_sem.at[kind])
        for kind, source in enumerate((master, first, second))
    ]
    for load in loads:
        load.start()

    barrier = pltpu.get_barrier_semaphore()

    def greet(to_inst, to_shard):
        pl.semaphore_signal(barrier, inc=1, device_id=(to_inst, to_shard), device_id_type=MESH)

    def greet_spot(step, carry):
        to = lax.rem(spot + step, spots) * 4
        for to_core in range(2):
            greet(near, to + 2 * flip + to_core)
            greet(inst, to + 2 * flip + to_core)
            greet(after, to + 2 * level + to_core)
            greet(before, to + 2 * level + to_core)

        @pl.when(step > 0)
        def _():
            for to_core in range(2):
                greet(inst, to + 2 * level + to_core)

        return carry

    lax.fori_loop(0, spots, greet_spot, 0)
    greet(inst, spot * 4 + 2 * level + 1 - core)
    greet(across, shard)

    for load in loads:
        load.wait()

    shape = (1, 1, 4, 2, 2, height, 128)
    at_spot = lax.broadcasted_iota(jnp.int32, shape, 2)
    at_level = lax.broadcasted_iota(jnp.int32, shape, 3)
    at_core = lax.broadcasted_iota(jnp.int32, shape, 4)
    line = lax.broadcasted_iota(jnp.int32, shape, 5)
    lane = lax.broadcasted_iota(jnp.int32, shape, 6)
    slice_0, slice_1 = table[2 * shard], table[2 * shard + 1]
    row_base = jnp.where((line & 1) == 0, slice_0 * 88, slice_1 * 88)
    width = 64 * height
    base = row_base + (at_spot * 4 + at_level * 2 + at_core) * width + (line >> 1) * 128 + lane
    blocks = spots // 4

    def weigh(step, carry):
        all_sum, master_sum = carry
        chunk = step // (n_inst * blocks)
        of_inst = lax.rem(step // blocks, n_inst)
        at = pl.ds(lax.rem(step, blocks) * 4, 4)
        key = mod_101(mod_101(base + step * (16 * width)) * 37) + 1
        key = key.astype(jnp.float32)
        m, f, s = (own[pl.ds(chunk, 1), pl.ds(of_inst, 1), at, :, :, kind] for kind in range(KINDS))
        term = m * key
        return all_sum + (term + (f + s) * key), master_sum + term

    zero = jnp.zeros(shape, jnp.float32)
    sums = lax.fori_loop(0, CHUNKS * n_inst * blocks, weigh, (zero, zero))
    of_mine = healthy[shard]
    both = jnp.stack([s.reshape(16 * height, 128).sum(axis=0) for s in sums])
    part[...] = jnp.where(of_mine == inst, both, 0.0)

    pl.semaphore_wait(barrier, 5 * n_shard // 2)

    for to_inst in (after, across, before):
        copy(part, part_got.at[inst], part_send, part_recv, to_inst, shard).start()
    part_got[inst] = part[...]

    def relays(chunk):
        return (
            (own.at[chunk, far, :, flip], cross_in.at[chunk, 0], 0, far),
            (own.at[chunk, across, :, flip], cross_in.at[chunk, 1], 1, near),
            (own.at[chunk, across, :, level, 0], level_in.at[chunk, 0], 2, after),
            (own.at[chunk, across, :, level, 1], level_in.at[chunk, 1], 3, before),
        )

    def relay(chunk):
        for source, target, which, to_inst in relays(chunk):
            copy(source, target, relay_send.at[chunk, which], relay_recv.at[chunk, which], to_inst, shard).start()

    def spread_to(chunk, source, slot, to_inst, to_shard):
        copy(
            source, got[chunk].at[slot * n_shard + shard],
            spread_send.at[chunk], spread_recv.at[chunk], to_inst, to_shard,
        ).start()

    def spread_own(chunk):
        got[chunk][shard] = own[chunk, inst, spot, level, core]
        partner = 1 - core
        spread_to(chunk, own.at[chunk, inst, spot, level, partner], 0, inst, spot * 4 + 2 * level + partner)

        def spread(step, carry):
            to = lax.rem(spot + step, spots)
            to_shard = to * 4 + 2 * level
            spread_to(chunk, own.at[chunk, after, to, level, 1], 1, after, to_shard + 1)
            spread_to(chunk, own.at[chunk, before, to, level, 0], 2, before, to_shard)

            @pl.when(step > 0)
            def _():
                spread_to(chunk, own.at[chunk, inst, to, level, 0], 0, inst, to_shard)
                spread_to(chunk, own.at[chunk, inst, to, level, 1], 0, inst, to_shard + 1)

            return carry

        lax.fori_loop(0, spots, spread, 0)

    def mix(chunk):
        for _, target, which, _ in relays(chunk):
            waiting(target, relay_send.at[chunk, which], relay_recv.at[chunk, which]).wait_recv()

        def at_spots(step, carry):
            at = pl.ds(step * 4, 4)
            for which, from_inst, to_inst in ((0, near, inst), (1, far, near)):
                cross_out[chunk, which, at] = jnp.where(
                    of_mine == from_inst, cross_in[chunk, which, at], own[chunk, to_inst, at, flip]
                )
            for which, from_inst, to_inst in ((0, before, after), (1, after, before)):
                level_out[chunk, which, at] = jnp.where(
                    of_mine == from_inst, level_in[chunk, which, at], own[chunk, to_inst, at, level, which]
                )
            return carry

        lax.fori_loop(0, spots // 4, at_spots, 0)

    def spread_mixed(chunk):
        def spread(step, carry):
            to = lax.rem(spot + step, spots)
            for to_core in range(2):
                to_shard = to * 4 + 2 * flip + to_core
                spread_to(chunk, cross_out.at[chunk, 1, to, to_core], 2 - level, near, to_shard)
                spread_to(chunk, cross_out.at[chunk, 0, to, to_core], 0, inst, to_shard)
            to_shard = to * 4 + 2 * level
            spread_to(chunk, level_out.at[chunk, 0, to], 1, after, to_shard)
            spread_to(chunk, level_out.at[chunk, 1, to], 2, before, to_shard + 1)
            return carry

        lax.fori_loop(0, spots, spread, 0)

    relay(0)
    spread_own(0)
    for chunk in range(1, CHUNKS):
        relay(chunk)

    some = pl.ds(0, n_inst - 1)
    waiting(part_got.at[some], part_send, part_recv).wait()
    row[...] = part_got[...].sum(axis=0)
    side_at, place = shard // SIDE, lax.rem(shard, SIDE)

    def share_row(step, carry):
        to = lax.rem(place + step, SIDE)
        copy(row, row_got.at[place], row_send, row_recv, inst, side_at * SIDE + to).start()
        return carry

    lax.fori_loop(1, SIDE, share_row, 0)
    row_got[place] = row[...]

    for chunk in range(CHUNKS):
        mix(chunk)
        spread_mixed(chunk)
        if chunk + 1 < CHUNKS:
            spread_own(chunk + 1)

    rotation = table[0] >> 1
    came = pl.ds(0, 5 * n_shard // 2 - 1)

    def held(chunk, owner):
        turn = (healthy[owner] - inst) & 3
        of_level = (owner >> 1) & 1
        same = jnp.where(turn == 0, 0, jnp.where(turn == 3, 1, jnp.where(turn == 1, 2, 1 + core)))
        beside = jnp.where(of_level == 1, 1, 3)
        other = jnp.where((turn == 0) | (turn == beside), 0, 2 - of_level)
        slot = jnp.where(of_level == level, same, other)
        return got[chunk][slot * n_shard + owner]

    def deal(chunk):
        waiting(got[chunk].at[came], spread_send.at[chunk], spread_recv.at[chunk]).wait_recv()

        def stage(new, carry):
            low = held(chunk, (new - rotation - 1) & (n_shard - 1))
            high = held(chunk, (new - rotation) & (n_shard - 1))
            lines = []
            for at in range(0, height, 2):
                lines += [low[:, at + 1:at + 2], high[:, at:at + 1]]
            staged[chunk, new] = jnp.concatenate(lines, axis=1)
            return carry

        lax.fori_loop(0, n_shard, stage, 0)
        place_there = final.at[:, chunk, inst, spot, level, core]

        def deal_to(recv_sem, to_inst, to_shard):
            copy(staged.at[chunk, to_shard], place_there, deal_send.at[chunk], recv_sem, to_inst, to_shard).start()

        def deal_cross(step, carry):
            to = lax.rem(spot + step, spots) * 4 + 2 * flip
            for to_core in range(2):
                deal_to(pass_recv.at[chunk, 0], inst, to + to_core)
                deal_to(pass_recv.at[chunk, 1], near, to + to_core)
            return carry

        passing = lax.rem(inst + 3 + 2 * core, n_inst)
        resting = lax.rem(inst + 1 + 2 * core, n_inst)

        def deal_passed(step, carry):
            to = lax.rem(spot + step, spots) * 4 + 2 * level
            for to_core in range(2):
                deal_to(pass_recv.at[chunk, 2 + core], passing, to + to_core)
            return carry

        def deal_rest(step, carry):
            to = lax.rem(spot + step, spots) * 4 + 2 * level
            for to_core in range(2):
                deal_to(deal_recv.at[chunk], resting, to + to_core)

            @pl.when(step > 0)
            def _():
                for to_core in range(2):
                    deal_to(deal_recv.at[chunk], inst, to + to_core)

            return carry

        lax.fori_loop(0, spots, deal_cross, 0)
        lax.fori_loop(0, spots, deal_passed, 0)
        lax.fori_loop(0, spots, deal_rest, 0)
        deal_to(deal_recv.at[chunk], inst, spot * 4 + 2 * level + 1 - core)
        final[:, chunk, inst, spot, level, core] = staged[chunk, shard]

    def passes(chunk):
        return (
            (final.at[:, chunk, inst, :, flip], near),
            (final.at[:, chunk, near, :, flip], far),
            (final.at[:, chunk, after, :, level, 0], before),
            (final.at[:, chunk, before, :, level, 1], after),
        )

    def passed(chunk):
        return (
            final.at[:, chunk, far, :, flip],
            final.at[:, chunk, across, :, flip],
            final.at[:, chunk, across, :, level, 0],
            final.at[:, chunk, across, :, level, 1],
        )

    def pass_on(chunk):
        for which, (there, to_inst) in enumerate(passes(chunk)):
            waiting(there, deal_send.at[chunk], pass_recv.at[chunk, which]).wait_recv()
            copy(there, there, far_send.at[chunk, which], far_recv.at[chunk, which], to_inst, shard).start()

    for chunk in range(CHUNKS):
        deal(chunk)
        if chunk == 0:
            few = pl.ds(0, SIDE - 1)
            waiting(row_got.at[few], row_send, row_recv).wait()
            total[...] = row_got[...].sum(axis=0)

            def share_total(step, carry):
                to = lax.rem(side_at + step, SIDE)
                copy(total, total_got.at[side_at], total_send, total_recv, inst, to * SIDE + place).start()
                return carry

            lax.fori_loop(1, SIDE, share_total, 0)
            total_got[side_at] = total[...]
    for chunk in range(CHUNKS):
        pass_on(chunk)

    waiting(total_got.at[pl.ds(0, SIDE - 1)], total_send, total_recv).wait()
    sums_out[...] = total_got[...].sum(axis=0)

    rest = pl.ds(0, n_shard - 1)
    for chunk in range(CHUNKS):
        waiting(got[chunk].at[rest], deal_send.at[chunk], deal_recv.at[chunk]).wait_recv()
        for which, there in enumerate(passed(chunk)):
            waiting(there, far_send.at[chunk, which], far_recv.at[chunk, which]).wait_recv()
        pltpu.make_async_copy(final.at[:, chunk], out.at[:, chunk], store_sem.at[chunk]).start()
    for chunk in range(CHUNKS):
        waiting(got[chunk].at[came], spread_send.at[chunk], spread_recv.at[chunk]).wait_send()
        waiting(got[chunk].at[came], deal_send.at[chunk], deal_recv.at[chunk]).wait_send()
        for _, target, which, _ in relays(chunk):
            waiting(target, relay_send.at[chunk, which], relay_recv.at[chunk, which]).wait_send()
        for which, there in enumerate(passed(chunk)):
            waiting(there, far_send.at[chunk, which], far_recv.at[chunk, which]).wait_send()
        pltpu.make_async_copy(final.at[:, chunk], out.at[:, chunk], store_sem.at[chunk]).wait()


def on_device(n_inst, n_shard, master_old, first_old, second_old, healthy, slice_table):
    rows, columns = master_old.shape[1:]
    spots = n_shard // 4
    pieces = (CHUNKS, n_inst, spots, 2, 2)
    arrays = [to_pieces(a, pieces) for a in (master_old, first_old, second_old)]
    tile = arrays[0].shape[5:]
    anywhere = pl.BlockSpec(memory_space=pl.ANY)
    vmem = pl.BlockSpec(memory_space=pltpu.VMEM)
    smem = pl.BlockSpec(memory_space=pltpu.SMEM)
    dma = pltpu.SemaphoreType.DMA

    def buffer(*shape):
        return pltpu.VMEM((*shape, *tile), jnp.float32)

    def sums(*shape):
        return pltpu.VMEM((*shape, 2, 128), jnp.float32)

    out, checks = pl.pallas_call(
        functools.partial(kernel, n_inst, n_shard),
        out_shape=(
            jax.ShapeDtypeStruct((KINDS, *pieces, *tile), jnp.float32),
            jax.ShapeDtypeStruct((2, 128), jnp.float32),
        ),
        in_specs=[smem, smem, anywhere, anywhere, anywhere],
        out_specs=(anywhere, vmem),
        scratch_shapes=[
            buffer(*pieces, KINDS),
            buffer(CHUNKS, 2, spots, 2, KINDS),
            buffer(CHUNKS, 2, spots, 2, KINDS),
            buffer(CHUNKS, 2, spots, KINDS),
            buffer(CHUNKS, 2, spots, KINDS),
            buffer(CHUNKS, n_shard, KINDS),
            buffer(KINDS, *pieces),
            sums(), sums(n_inst), sums(), sums(SIDE), sums(), sums(SIDE),
            dma((KINDS,)),
            dma((CHUNKS, 4)), dma((CHUNKS, 4)),
            dma((CHUNKS,)), dma((CHUNKS,)),
            dma((CHUNKS,)), dma((CHUNKS,)), dma((CHUNKS, 4)),
            dma((CHUNKS, 4)), dma((CHUNKS, 4)),
            dma, dma, dma, dma, dma, dma,
            dma((CHUNKS,)),
            *[buffer(3 * n_shard, KINDS) for _ in range(CHUNKS)],
        ],
        compiler_params=pltpu.CompilerParams(collective_id=0, has_side_effects=True),
    )(healthy, slice_table, *arrays)
    master, first_moment, second = (from_pieces(out[k], rows, columns) for k in range(KINDS))
    checksum = jnp.sum(checks, axis=1).reshape(1, 2) * (1.0 / (101.0 * 2.0 * columns))
    return master, first_moment, second, master.astype(jnp.bfloat16), checksum


def solution(mesh):
    per_slice = P("inst", "shard", None)
    return jax.shard_map(
        functools.partial(on_device, mesh.shape["inst"], mesh.shape["shard"]),
        mesh=mesh,
        in_specs=(per_slice, per_slice, per_slice, P(), P()),
        out_specs=(per_slice, per_slice, per_slice, per_slice, P("inst", None)),
        check_vma=False,
    )
```

```python
import functools
import math

import jax
import jax.numpy as jnp
from jax import lax
from jax.experimental import pallas as pl
from jax.experimental.pallas import tpu as pltpu
from jax.sharding import PartitionSpec as P

MESH = pl.DeviceIdType.MESH
KINDS = 3
CHUNKS = 2
SIDE = 8


def to_pieces(shard, pieces):
    rows, columns = shard.shape[1:]
    lines = shard.reshape(rows, columns // 128, 128).transpose(1, 0, 2)
    return lines.reshape(*pieces, rows * columns // (128 * math.prod(pieces)), 128)


def from_pieces(pieces, rows, columns):
    lines = pieces.reshape(columns // 128, rows, 128)
    return lines.transpose(1, 0, 2).reshape(1, rows, columns)


def mod_101(x):
    return x - ((x * 10382) >> 20) * 101


def kernel(n_inst, n_shard, healthy, table, master, first, second, final, sums_out,
           own, cross_in, cross_out, level_in, level_out, staged,
           part, part_got, row, row_got, total, total_got,
           load_sem, relay_send, relay_recv, spread_send, spread_recv,
           deal_send, deal_recv, pass_recv, far_send, far_recv,
           part_send, part_recv, row_send, row_recv, total_send, total_recv, *got):
    inst = lax.axis_index("inst")
    shard = lax.axis_index("shard")
    spots = n_shard // 4
    spot, level, core = shard // 4, lax.rem(shard // 2, 2), lax.rem(shard, 2)
    flip = 1 - level
    height = own.shape[6]
    after = lax.rem(inst + 1, n_inst)
    across = lax.rem(inst + 2, n_inst)
    before = lax.rem(inst + 3, n_inst)
    near = lax.rem(inst + 3 + 2 * level, n_inst)
    far = lax.rem(inst + 1 + 2 * level, n_inst)

    def copy(source, target, send_sem, recv_sem, to_inst, to_shard):
        return pltpu.make_async_remote_copy(
            src_ref=source,
            dst_ref=target,
            send_sem=send_sem,
            recv_sem=recv_sem,
            device_id=(to_inst, to_shard),
            device_id_type=MESH,
        )

    def waiting(target, send_sem, recv_sem):
        return copy(target, target, send_sem, recv_sem, inst, shard)

    loads = [
        pltpu.make_async_copy(source, own.at[:, :, :, :, :, kind], load_sem.at[kind])
        for kind, source in enumerate((master, first, second))
    ]
    for load in loads:
        load.start()

    barrier = pltpu.get_barrier_semaphore()

    def greet(to_inst, to_shard):
        pl.semaphore_signal(barrier, inc=1, device_id=(to_inst, to_shard), device_id_type=MESH)

    def greet_spot(step, carry):
        to = lax.rem(spot + step, spots) * 4
        for to_core in range(2):
            greet(near, to + 2 * flip + to_core)
            greet(inst, to + 2 * flip + to_core)
            greet(after, to + 2 * level + to_core)
            greet(before, to + 2 * level + to_core)

        @pl.when(step > 0)
        def _():
            for to_core in range(2):
                greet(inst, to + 2 * level + to_core)

        return carry

    lax.fori_loop(0, spots, greet_spot, 0)
    greet(inst, spot * 4 + 2 * level + 1 - core)
    greet(across, shard)

    for load in loads:
        load.wait()

    shape = (1, 1, 4, 2, 2, height, 128)
    at_spot = lax.broadcasted_iota(jnp.int32, shape, 2)
    at_level = lax.broadcasted_iota(jnp.int32, shape, 3)
    at_core = lax.broadcasted_iota(jnp.int32, shape, 4)
    line = lax.broadcasted_iota(jnp.int32, shape, 5)
    lane = lax.broadcasted_iota(jnp.int32, shape, 6)
    slice_0, slice_1 = table[2 * shard], table[2 * shard + 1]
    row_base = jnp.where((line & 1) == 0, slice_0 * 88, slice_1 * 88)
    width = 64 * height
    base = row_base + (at_spot * 4 + at_level * 2 + at_core) * width + (line >> 1) * 128 + lane
    blocks = spots // 4

    def weigh(step, carry):
        all_sum, master_sum = carry
        chunk = step // (n_inst * blocks)
        of_inst = lax.rem(step // blocks, n_inst)
        at = pl.ds(lax.rem(step, blocks) * 4, 4)
        key = mod_101(mod_101(base + step * (16 * width)) * 37) + 1
        key = key.astype(jnp.float32)
        m, f, s = (own[pl.ds(chunk, 1), pl.ds(of_inst, 1), at, :, :, kind] for kind in range(KINDS))
        term = m * key
        return all_sum + (term + (f + s) * key), master_sum + term

    zero = jnp.zeros(shape, jnp.float32)
    sums = lax.fori_loop(0, CHUNKS * n_inst * blocks, weigh, (zero, zero))
    of_mine = healthy[shard]
    both = jnp.stack([s.reshape(16 * height, 128).sum(axis=0) for s in sums])
    part[...] = jnp.where(of_mine == inst, both, 0.0)

    pl.semaphore_wait(barrier, 5 * n_shard // 2)

    for to_inst in (after, across, before):
        copy(part, part_got.at[inst], part_send, part_recv, to_inst, shard).start()
    part_got[inst] = part[...]

    def relays(chunk):
        return (
            (own.at[chunk, far, :, flip], cross_in.at[chunk, 0], 0, far),
            (own.at[chunk, across, :, flip], cross_in.at[chunk, 1], 1, near),
            (own.at[chunk, across, :, level, 0], level_in.at[chunk, 0], 2, after),
            (own.at[chunk, across, :, level, 1], level_in.at[chunk, 1], 3, before),
        )

    def relay(chunk):
        for source, target, which, to_inst in relays(chunk):
            copy(source, target, relay_send.at[chunk, which], relay_recv.at[chunk, which], to_inst, shard).start()

    def spread_to(chunk, source, slot, to_inst, to_shard):
        copy(
            source, got[chunk].at[slot * n_shard + shard],
            spread_send.at[chunk], spread_recv.at[chunk], to_inst, to_shard,
        ).start()

    def spread_own(chunk):
        got[chunk][shard] = own[chunk, inst, spot, level, core]
        partner = 1 - core
        spread_to(chunk, own.at[chunk, inst, spot, level, partner], 0, inst, spot * 4 + 2 * level + partner)

        def spread(step, carry):
            to = lax.rem(spot + step, spots)
            to_shard = to * 4 + 2 * level
            spread_to(chunk, own.at[chunk, after, to, level, 1], 1, after, to_shard + 1)
            spread_to(chunk, own.at[chunk, before, to, level, 0], 2, before, to_shard)

            @pl.when(step > 0)
            def _():
                spread_to(chunk, own.at[chunk, inst, to, level, 0], 0, inst, to_shard)
                spread_to(chunk, own.at[chunk, inst, to, level, 1], 0, inst, to_shard + 1)

            return carry

        lax.fori_loop(0, spots, spread, 0)

    def mix(chunk):
        for _, target, which, _ in relays(chunk):
            waiting(target, relay_send.at[chunk, which], relay_recv.at[chunk, which]).wait_recv()

        def at_spots(step, carry):
            at = pl.ds(step * 4, 4)
            for which, from_inst, to_inst in ((0, near, inst), (1, far, near)):
                cross_out[chunk, which, at] = jnp.where(
                    of_mine == from_inst, cross_in[chunk, which, at], own[chunk, to_inst, at, flip]
                )
            for which, from_inst, to_inst in ((0, before, after), (1, after, before)):
                level_out[chunk, which, at] = jnp.where(
                    of_mine == from_inst, level_in[chunk, which, at], own[chunk, to_inst, at, level, which]
                )
            return carry

        lax.fori_loop(0, spots // 4, at_spots, 0)

    def spread_mixed(chunk):
        def spread(step, carry):
            to = lax.rem(spot + step, spots)
            for to_core in range(2):
                to_shard = to * 4 + 2 * flip + to_core
                spread_to(chunk, cross_out.at[chunk, 1, to, to_core], 2 - level, near, to_shard)
                spread_to(chunk, cross_out.at[chunk, 0, to, to_core], 0, inst, to_shard)
            to_shard = to * 4 + 2 * level
            spread_to(chunk, level_out.at[chunk, 0, to], 1, after, to_shard)
            spread_to(chunk, level_out.at[chunk, 1, to], 2, before, to_shard + 1)
            return carry

        lax.fori_loop(0, spots, spread, 0)

    relay(0)
    spread_own(0)
    for chunk in range(1, CHUNKS):
        relay(chunk)

    some = pl.ds(0, n_inst - 1)
    waiting(part_got.at[some], part_send, part_recv).wait()
    row[...] = part_got[...].sum(axis=0)
    side_at, place = shard // SIDE, lax.rem(shard, SIDE)

    def share_row(step, carry):
        to = lax.rem(place + step, SIDE)
        copy(row, row_got.at[place], row_send, row_recv, inst, side_at * SIDE + to).start()
        return carry

    lax.fori_loop(1, SIDE, share_row, 0)
    row_got[place] = row[...]

    for chunk in range(CHUNKS):
        mix(chunk)
        spread_mixed(chunk)
        if chunk + 1 < CHUNKS:
            spread_own(chunk + 1)

    rotation = table[0] >> 1
    came = pl.ds(0, 5 * n_shard // 2 - 1)

    def held(chunk, owner):
        turn = (healthy[owner] - inst) & 3
        of_level = (owner >> 1) & 1
        same = jnp.where(turn == 0, 0, jnp.where(turn == 3, 1, jnp.where(turn == 1, 2, 1 + core)))
        beside = jnp.where(of_level == 1, 1, 3)
        other = jnp.where((turn == 0) | (turn == beside), 0, 2 - of_level)
        slot = jnp.where(of_level == level, same, other)
        return got[chunk][slot * n_shard + owner]

    def deal(chunk):
        waiting(got[chunk].at[came], spread_send.at[chunk], spread_recv.at[chunk]).wait_recv()

        def stage(new, carry):
            low = held(chunk, (new - rotation - 1) & (n_shard - 1))
            high = held(chunk, (new - rotation) & (n_shard - 1))
            lines = []
            for at in range(0, height, 2):
                lines += [low[:, at + 1:at + 2], high[:, at:at + 1]]
            staged[chunk, new] = jnp.concatenate(lines, axis=1)
            return carry

        lax.fori_loop(0, n_shard, stage, 0)
        place_there = final.at[:, chunk, inst, spot, level, core]

        def deal_to(recv_sem, to_inst, to_shard):
            copy(staged.at[chunk, to_shard], place_there, deal_send.at[chunk], recv_sem, to_inst, to_shard).start()

        def deal_cross(step, carry):
            to = lax.rem(spot + step, spots) * 4 + 2 * flip
            for to_core in range(2):
                deal_to(pass_recv.at[chunk, 0], inst, to + to_core)
                deal_to(pass_recv.at[chunk, 1], near, to + to_core)
            return carry

        passing = lax.rem(inst + 3 + 2 * core, n_inst)
        resting = lax.rem(inst + 1 + 2 * core, n_inst)

        def deal_passed(step, carry):
            to = lax.rem(spot + step, spots) * 4 + 2 * level
            for to_core in range(2):
                deal_to(pass_recv.at[chunk, 2 + core], passing, to + to_core)
            return carry

        def deal_rest(step, carry):
            to = lax.rem(spot + step, spots) * 4 + 2 * level
            for to_core in range(2):
                deal_to(deal_recv.at[chunk], resting, to + to_core)

            @pl.when(step > 0)
            def _():
                for to_core in range(2):
                    deal_to(deal_recv.at[chunk], inst, to + to_core)

            return carry

        lax.fori_loop(0, spots, deal_cross, 0)
        lax.fori_loop(0, spots, deal_passed, 0)
        lax.fori_loop(0, spots, deal_rest, 0)
        deal_to(deal_recv.at[chunk], inst, spot * 4 + 2 * level + 1 - core)
        final[:, chunk, inst, spot, level, core] = staged[chunk, shard]

    def passes(chunk):
        return (
            (final.at[:, chunk, inst, :, flip], near),
            (final.at[:, chunk, near, :, flip], far),
            (final.at[:, chunk, after, :, level, 0], before),
            (final.at[:, chunk, before, :, level, 1], after),
        )

    def passed(chunk):
        return (
            final.at[:, chunk, far, :, flip],
            final.at[:, chunk, across, :, flip],
            final.at[:, chunk, across, :, level, 0],
            final.at[:, chunk, across, :, level, 1],
        )

    def pass_on(chunk):
        for which, (there, to_inst) in enumerate(passes(chunk)):
            waiting(there, deal_send.at[chunk], pass_recv.at[chunk, which]).wait_recv()
            copy(there, there, far_send.at[chunk, which], far_recv.at[chunk, which], to_inst, shard).start()

    for chunk in range(CHUNKS):
        deal(chunk)
        if chunk == 0:
            few = pl.ds(0, SIDE - 1)
            waiting(row_got.at[few], row_send, row_recv).wait()
            total[...] = row_got[...].sum(axis=0)

            def share_total(step, carry):
                to = lax.rem(side_at + step, SIDE)
                copy(total, total_got.at[side_at], total_send, total_recv, inst, to * SIDE + place).start()
                return carry

            lax.fori_loop(1, SIDE, share_total, 0)
            total_got[side_at] = total[...]
    for chunk in range(CHUNKS):
        pass_on(chunk)

    waiting(total_got.at[pl.ds(0, SIDE - 1)], total_send, total_recv).wait()
    sums_out[...] = total_got[...].sum(axis=0)

    rest = pl.ds(0, n_shard - 1)
    for chunk in range(CHUNKS):
        waiting(got[chunk].at[rest], deal_send.at[chunk], deal_recv.at[chunk]).wait_recv()
        for which, there in enumerate(passed(chunk)):
            waiting(there, far_send.at[chunk, which], far_recv.at[chunk, which]).wait_recv()
    for chunk in range(CHUNKS):
        waiting(got[chunk].at[came], spread_send.at[chunk], spread_recv.at[chunk]).wait_send()
        waiting(got[chunk].at[came], deal_send.at[chunk], deal_recv.at[chunk]).wait_send()
        for _, target, which, _ in relays(chunk):
            waiting(target, relay_send.at[chunk, which], relay_recv.at[chunk, which]).wait_send()
        for which, there in enumerate(passed(chunk)):
            waiting(there, far_send.at[chunk, which], far_recv.at[chunk, which]).wait_send()


def finish(scale, state, checks, master, first, second, half, checksum, halved, sem):
    stores = [
        pltpu.make_async_copy(state.at[kind], target, sem.at[kind])
        for kind, target in enumerate((master, first, second))
    ]
    for store in stores:
        store.start()
    tiles = state.shape[1]

    def narrow(step, carry):
        for tile in range(8):
            at = pl.ds(pl.multiple_of((step * 8 + tile) * 128, 128), 128)
            halved[0, :, at] = state[0, step * 8 + tile].astype(jnp.bfloat16)
        return carry

    lax.fori_loop(0, tiles // 8, narrow, 0)
    last = pltpu.make_async_copy(halved, half, sem.at[KINDS])
    last.start()
    checksum[...] = checks[...].sum(axis=1).reshape(1, 2) * scale
    for store in stores:
        store.wait()
    last.wait()


def on_device(n_inst, n_shard, master_old, first_old, second_old, healthy, slice_table):
    rows, columns = master_old.shape[1:]
    spots = n_shard // 4
    pieces = (CHUNKS, n_inst, spots, 2, 2)
    arrays = [to_pieces(a, pieces) for a in (master_old, first_old, second_old)]
    healthy, slice_table, *arrays = (
        pltpu.with_memory_space_constraint(a, pltpu.HBM) for a in (healthy, slice_table, *arrays)
    )
    tile = arrays[0].shape[5:]
    anywhere = pl.BlockSpec(memory_space=pltpu.HBM)
    vmem = pl.BlockSpec(memory_space=pltpu.VMEM)
    smem = pl.BlockSpec(memory_space=pltpu.SMEM)
    dma = pltpu.SemaphoreType.DMA

    def buffer(*shape):
        return pltpu.VMEM((*shape, *tile), jnp.float32)

    def sums(*shape):
        return pltpu.VMEM((*shape, 2, 128), jnp.float32)

    out, checks = pl.pallas_call(
        functools.partial(kernel, n_inst, n_shard),
        out_shape=(
            jax.ShapeDtypeStruct((KINDS, *pieces, *tile), jnp.float32),
            jax.ShapeDtypeStruct((2, 128), jnp.float32),
        ),
        in_specs=[smem, smem, anywhere, anywhere, anywhere],
        out_specs=(vmem, vmem),
        scratch_shapes=[
            buffer(*pieces, KINDS),
            buffer(CHUNKS, 2, spots, 2, KINDS),
            buffer(CHUNKS, 2, spots, 2, KINDS),
            buffer(CHUNKS, 2, spots, KINDS),
            buffer(CHUNKS, 2, spots, KINDS),
            buffer(CHUNKS, n_shard, KINDS),
            sums(), sums(n_inst), sums(), sums(SIDE), sums(), sums(SIDE),
            dma((KINDS,)),
            dma((CHUNKS, 4)), dma((CHUNKS, 4)),
            dma((CHUNKS,)), dma((CHUNKS,)),
            dma((CHUNKS,)), dma((CHUNKS,)), dma((CHUNKS, 4)),
            dma((CHUNKS, 4)), dma((CHUNKS, 4)),
            dma, dma, dma, dma, dma, dma,
            *[buffer(3 * n_shard, KINDS) for _ in range(CHUNKS)],
        ],
        compiler_params=pltpu.CompilerParams(collective_id=0, has_side_effects=True, vmem_limit_bytes=16 << 20),
    )(healthy, slice_table, *arrays)
    state = jax.ShapeDtypeStruct((columns // 128, rows, 128), jnp.float32)
    *outs, half, checksum = pl.pallas_call(
        functools.partial(finish, 1.0 / (101.0 * 2.0 * columns)),
        out_shape=(
            state, state, state,
            jax.ShapeDtypeStruct((1, rows, columns), jnp.bfloat16),
            jax.ShapeDtypeStruct((1, 2), jnp.float32),
        ),
        in_specs=[vmem, vmem],
        out_specs=(*[pl.BlockSpec(memory_space=pltpu.HBM)] * 4, vmem),
        scratch_shapes=[pltpu.VMEM((1, rows, columns), jnp.bfloat16), dma((KINDS + 1,))],
        compiler_params=pltpu.CompilerParams(vmem_limit_bytes=4 << 20),
    )(out.reshape(KINDS, columns // 128, rows, 128), checks)
    return *(from_pieces(a, rows, columns) for a in outs), half, checksum


def solution(mesh):
    per_slice = P("inst", "shard", None)
    return jax.shard_map(
        functools.partial(on_device, mesh.shape["inst"], mesh.shape["shard"]),
        mesh=mesh,
        in_specs=(per_slice, per_slice, per_slice, P(), P()),
        out_specs=(per_slice, per_slice, per_slice, per_slice, P("inst", None)),
        check_vma=False,
    )
```

```python
import functools
import math

import jax
import jax.numpy as jnp
from jax import lax
from jax.experimental import pallas as pl
from jax.experimental.pallas import tpu as pltpu
from jax.sharding import PartitionSpec as P

MESH = pl.DeviceIdType.MESH
KINDS = 3
CHUNKS = 2
SIDE = 8


def to_pieces(shard, pieces):
    rows, columns = shard.shape[1:]
    lines = shard.reshape(rows, columns // 128, 128).transpose(1, 0, 2)
    return lines.reshape(*pieces, rows * columns // (128 * math.prod(pieces)), 128)


def from_pieces(pieces, rows, columns):
    lines = pieces.reshape(columns // 128, rows, 128)
    return lines.transpose(1, 0, 2).reshape(1, rows, columns)


def mod_101(x):
    return x - ((x * 10382) >> 20) * 101


def kernel(n_inst, n_shard, healthy_in, table_in, master, first, second, final, sums_out,
           own, cross_in, cross_out, level_in, level_out, staged,
           part, part_got, row, row_got, total, total_got,
           healthy, table, load_sem, relay_send, relay_recv, spread_send, spread_recv,
           deal_send, deal_recv, pass_recv, far_send, far_recv,
           part_send, part_recv, row_send, row_recv, total_send, total_recv, *got):
    inst = lax.axis_index("inst")
    shard = lax.axis_index("shard")
    spots = n_shard // 4
    spot, level, core = shard // 4, lax.rem(shard // 2, 2), lax.rem(shard, 2)
    flip = 1 - level
    height = own.shape[6]
    after = lax.rem(inst + 1, n_inst)
    across = lax.rem(inst + 2, n_inst)
    before = lax.rem(inst + 3, n_inst)
    near = lax.rem(inst + 3 + 2 * level, n_inst)
    far = lax.rem(inst + 1 + 2 * level, n_inst)

    def copy(source, target, send_sem, recv_sem, to_inst, to_shard):
        return pltpu.make_async_remote_copy(
            src_ref=source,
            dst_ref=target,
            send_sem=send_sem,
            recv_sem=recv_sem,
            device_id=(to_inst, to_shard),
            device_id_type=MESH,
        )

    def waiting(target, send_sem, recv_sem):
        return copy(target, target, send_sem, recv_sem, inst, shard)

    loads = [
        pltpu.make_async_copy(source, own.at[:, :, :, :, :, kind], load_sem.at[kind])
        for kind, source in enumerate((master, first, second))
    ]
    loads += [
        pltpu.make_async_copy(healthy_in, healthy, load_sem.at[KINDS]),
        pltpu.make_async_copy(table_in, table, load_sem.at[KINDS + 1]),
    ]
    for load in loads:
        load.start()

    barrier = pltpu.get_barrier_semaphore()

    def greet(to_inst, to_shard):
        pl.semaphore_signal(barrier, inc=1, device_id=(to_inst, to_shard), device_id_type=MESH)

    def greet_spot(step, carry):
        to_y = lax.rem(spot // 4 + 6 - step // 4, 4)
        to_x = lax.rem(lax.rem(spot, 4) + 6 - lax.rem(step, 4), 4)
        to = (to_y * 4 + to_x) * 4
        for to_core in range(2):
            greet(near, to + 2 * flip + to_core)
            greet(after, to + 2 * level + to_core)
            greet(before, to + 2 * level + to_core)
            greet(inst, to + 2 * flip + to_core)

        @pl.when(to != spot * 4)
        def _():
            for to_core in range(2):
                greet(inst, to + 2 * level + to_core)

        return carry

    lax.fori_loop(0, spots, greet_spot, 0)
    greet(inst, spot * 4 + 2 * level + 1 - core)
    greet(across, shard)

    for load in loads:
        load.wait()

    shape = (1, 1, 4, 2, 2, height, 128)
    at_spot = lax.broadcasted_iota(jnp.int32, shape, 2)
    at_level = lax.broadcasted_iota(jnp.int32, shape, 3)
    at_core = lax.broadcasted_iota(jnp.int32, shape, 4)
    line = lax.broadcasted_iota(jnp.int32, shape, 5)
    lane = lax.broadcasted_iota(jnp.int32, shape, 6)
    slice_0, slice_1 = table[2 * shard], table[2 * shard + 1]
    row_base = jnp.where((line & 1) == 0, slice_0 * 88, slice_1 * 88)
    width = 64 * height
    base = row_base + (at_spot * 4 + at_level * 2 + at_core) * width + (line >> 1) * 128 + lane
    blocks = spots // 4

    def weigh(step, carry):
        all_sum, master_sum = carry
        chunk = step // (n_inst * blocks)
        of_inst = lax.rem(step // blocks, n_inst)
        at = pl.ds(lax.rem(step, blocks) * 4, 4)
        key = mod_101(mod_101(base + step * (16 * width)) * 37) + 1
        key = key.astype(jnp.float32)
        m, f, s = (own[pl.ds(chunk, 1), pl.ds(of_inst, 1), at, :, :, kind] for kind in range(KINDS))
        term = m * key
        return all_sum + (term + (f + s) * key), master_sum + term

    zero = jnp.zeros(shape, jnp.float32)
    sums = lax.fori_loop(0, CHUNKS * n_inst * blocks, weigh, (zero, zero))
    of_mine = healthy[shard]
    both = jnp.stack([s.reshape(16 * height, 128).sum(axis=0) for s in sums])
    part[...] = jnp.where(of_mine == inst, both, 0.0)

    pl.semaphore_wait(barrier, 5 * n_shard // 2)

    for to_inst in (after, across, before):
        copy(part, part_got.at[inst], part_send, part_recv, to_inst, shard).start()
    part_got[inst] = part[...]

    def relays(chunk):
        return (
            (own.at[chunk, far, :, flip], cross_in.at[chunk, 0], 0, far),
            (own.at[chunk, across, :, flip], cross_in.at[chunk, 1], 1, near),
            (own.at[chunk, across, :, level, 0], level_in.at[chunk, 0], 2, after),
            (own.at[chunk, across, :, level, 1], level_in.at[chunk, 1], 3, before),
        )

    def relay(chunk):
        for source, target, which, to_inst in relays(chunk):
            copy(source, target, relay_send.at[chunk, which], relay_recv.at[chunk, which], to_inst, shard).start()

    def spread_to(chunk, source, slot, to_inst, to_shard):
        copy(
            source, got[chunk].at[slot * n_shard + shard],
            spread_send.at[chunk], spread_recv.at[chunk], to_inst, to_shard,
        ).start()

    def spread_own(chunk):
        got[chunk][shard] = own[chunk, inst, spot, level, core]
        partner = 1 - core
        spread_to(chunk, own.at[chunk, inst, spot, level, partner], 0, inst, spot * 4 + 2 * level + partner)

        def spread(step, carry):
            to = lax.rem(spot + step, spots)
            to_shard = to * 4 + 2 * level
            spread_to(chunk, own.at[chunk, after, to, level, 1], 1, after, to_shard + 1)
            spread_to(chunk, own.at[chunk, before, to, level, 0], 2, before, to_shard)

            @pl.when(step > 0)
            def _():
                spread_to(chunk, own.at[chunk, inst, to, level, 0], 0, inst, to_shard)
                spread_to(chunk, own.at[chunk, inst, to, level, 1], 0, inst, to_shard + 1)

            return carry

        lax.fori_loop(0, spots, spread, 0)

    def mix(chunk):
        for _, target, which, _ in relays(chunk):
            waiting(target, relay_send.at[chunk, which], relay_recv.at[chunk, which]).wait_recv()

        def at_spots(step, carry):
            at = pl.ds(step * 4, 4)
            for which, from_inst, to_inst in ((0, near, inst), (1, far, near)):
                cross_out[chunk, which, at] = jnp.where(
                    of_mine == from_inst, cross_in[chunk, which, at], own[chunk, to_inst, at, flip]
                )
            for which, from_inst, to_inst in ((0, before, after), (1, after, before)):
                level_out[chunk, which, at] = jnp.where(
                    of_mine == from_inst, level_in[chunk, which, at], own[chunk, to_inst, at, level, which]
                )
            return carry

        lax.fori_loop(0, spots // 4, at_spots, 0)

    def spread_mixed(chunk):
        def spread(step, carry):
            to = lax.rem(spot + step, spots)
            for to_core in range(2):
                to_shard = to * 4 + 2 * flip + to_core
                spread_to(chunk, cross_out.at[chunk, 1, to, to_core], 2 - level, near, to_shard)
                spread_to(chunk, cross_out.at[chunk, 0, to, to_core], 0, inst, to_shard)
            to_shard = to * 4 + 2 * level
            spread_to(chunk, level_out.at[chunk, 0, to], 1, after, to_shard)
            spread_to(chunk, level_out.at[chunk, 1, to], 2, before, to_shard + 1)
            return carry

        lax.fori_loop(0, spots, spread, 0)

    relay(0)
    spread_own(0)
    for chunk in range(1, CHUNKS):
        relay(chunk)

    some = pl.ds(0, n_inst - 1)
    waiting(part_got.at[some], part_send, part_recv).wait()
    row[...] = part_got[...].sum(axis=0)
    side_at, place = shard // SIDE, lax.rem(shard, SIDE)

    def share_row(step, carry):
        to = lax.rem(place + step, SIDE)
        copy(row, row_got.at[place], row_send, row_recv, inst, side_at * SIDE + to).start()
        return carry

    lax.fori_loop(1, SIDE, share_row, 0)
    row_got[place] = row[...]

    for chunk in range(CHUNKS):
        mix(chunk)
        spread_mixed(chunk)
        if chunk + 1 < CHUNKS:
            spread_own(chunk + 1)

    rotation = table[0] >> 1
    came = pl.ds(0, 5 * n_shard // 2 - 1)

    def held(chunk, owner):
        turn = (healthy[owner] - inst) & 3
        of_level = (owner >> 1) & 1
        same = jnp.where(turn == 0, 0, jnp.where(turn == 3, 1, jnp.where(turn == 1, 2, 1 + core)))
        beside = jnp.where(of_level == 1, 1, 3)
        other = jnp.where((turn == 0) | (turn == beside), 0, 2 - of_level)
        slot = jnp.where(of_level == level, same, other)
        return got[chunk][slot * n_shard + owner]

    def deal(chunk):
        waiting(got[chunk].at[came], spread_send.at[chunk], spread_recv.at[chunk]).wait_recv()

        def stage(new, carry):
            low = held(chunk, (new - rotation - 1) & (n_shard - 1))
            high = held(chunk, (new - rotation) & (n_shard - 1))
            lines = []
            for at in range(0, height, 2):
                lines += [low[:, at + 1:at + 2], high[:, at:at + 1]]
            staged[chunk, new] = jnp.concatenate(lines, axis=1)
            return carry

        lax.fori_loop(0, n_shard, stage, 0)
        place_there = final.at[:, chunk, inst, spot, level, core]

        def deal_to(recv_sem, to_inst, to_shard):
            copy(staged.at[chunk, to_shard], place_there, deal_send.at[chunk], recv_sem, to_inst, to_shard).start()

        def deal_cross(step, carry):
            to = lax.rem(spot + step, spots) * 4 + 2 * flip
            for to_core in range(2):
                deal_to(pass_recv.at[chunk, 0], inst, to + to_core)
                deal_to(pass_recv.at[chunk, 1], near, to + to_core)
            return carry

        passing = lax.rem(inst + 3 + 2 * core, n_inst)
        resting = lax.rem(inst + 1 + 2 * core, n_inst)

        def deal_passed(step, carry):
            to = lax.rem(spot + step, spots) * 4 + 2 * level
            for to_core in range(2):
                deal_to(pass_recv.at[chunk, 2 + core], passing, to + to_core)
            return carry

        def deal_rest(step, carry):
            to = lax.rem(spot + step, spots) * 4 + 2 * level
            for to_core in range(2):
                deal_to(deal_recv.at[chunk], resting, to + to_core)

            @pl.when(step > 0)
            def _():
                for to_core in range(2):
                    deal_to(deal_recv.at[chunk], inst, to + to_core)

            return carry

        lax.fori_loop(0, spots, deal_cross, 0)
        lax.fori_loop(0, spots, deal_passed, 0)
        lax.fori_loop(0, spots, deal_rest, 0)
        deal_to(deal_recv.at[chunk], inst, spot * 4 + 2 * level + 1 - core)
        final[:, chunk, inst, spot, level, core] = staged[chunk, shard]

    def passes(chunk):
        return (
            (final.at[:, chunk, inst, :, flip], near),
            (final.at[:, chunk, near, :, flip], far),
            (final.at[:, chunk, after, :, level, 0], before),
            (final.at[:, chunk, before, :, level, 1], after),
        )

    def passed(chunk):
        return (
            final.at[:, chunk, far, :, flip],
            final.at[:, chunk, across, :, flip],
            final.at[:, chunk, across, :, level, 0],
            final.at[:, chunk, across, :, level, 1],
        )

    def pass_on(chunk):
        for which, (there, to_inst) in enumerate(passes(chunk)):
            waiting(there, deal_send.at[chunk], pass_recv.at[chunk, which]).wait_recv()
            copy(there, there, far_send.at[chunk, which], far_recv.at[chunk, which], to_inst, shard).start()

    for chunk in range(CHUNKS):
        deal(chunk)
        if chunk == 0:
            few = pl.ds(0, SIDE - 1)
            waiting(row_got.at[few], row_send, row_recv).wait()
            total[...] = row_got[...].sum(axis=0)

            def share_total(step, carry):
                to = lax.rem(side_at + step, SIDE)
                copy(total, total_got.at[side_at], total_send, total_recv, inst, to * SIDE + place).start()
                return carry

            lax.fori_loop(1, SIDE, share_total, 0)
            total_got[side_at] = total[...]
    for chunk in range(CHUNKS):
        pass_on(chunk)

    waiting(total_got.at[pl.ds(0, SIDE - 1)], total_send, total_recv).wait()
    sums_out[...] = total_got[...].sum(axis=0)

    rest = pl.ds(0, n_shard - 1)
    for chunk in range(CHUNKS):
        waiting(got[chunk].at[rest], deal_send.at[chunk], deal_recv.at[chunk]).wait_recv()
        for which, there in enumerate(passed(chunk)):
            waiting(there, far_send.at[chunk, which], far_recv.at[chunk, which]).wait_recv()
    for chunk in range(CHUNKS):
        waiting(got[chunk].at[came], spread_send.at[chunk], spread_recv.at[chunk]).wait_send()
        waiting(got[chunk].at[came], deal_send.at[chunk], deal_recv.at[chunk]).wait_send()
        for _, target, which, _ in relays(chunk):
            waiting(target, relay_send.at[chunk, which], relay_recv.at[chunk, which]).wait_send()
        for which, there in enumerate(passed(chunk)):
            waiting(there, far_send.at[chunk, which], far_recv.at[chunk, which]).wait_send()


def finish(scale, state, checks, master, first, second, half, checksum, halved, sem):
    stores = [
        pltpu.make_async_copy(state.at[kind], target, sem.at[kind])
        for kind, target in enumerate((master, first, second))
    ]
    for store in stores:
        store.start()
    tiles = state.shape[1]

    def narrow(step, carry):
        for tile in range(8):
            at = pl.ds(pl.multiple_of((step * 8 + tile) * 128, 128), 128)
            halved[0, :, at] = state[0, step * 8 + tile].astype(jnp.bfloat16)
        return carry

    lax.fori_loop(0, tiles // 8, narrow, 0, unroll=4)
    last = pltpu.make_async_copy(halved, half, sem.at[KINDS])
    last.start()
    checksum[...] = checks[...].sum(axis=1).reshape(1, 2) * scale
    for store in stores:
        store.wait()
    last.wait()


def on_device(n_inst, n_shard, master_old, first_old, second_old, healthy, slice_table):
    rows, columns = master_old.shape[1:]
    spots = n_shard // 4
    pieces = (CHUNKS, n_inst, spots, 2, 2)
    arrays = [to_pieces(a, pieces) for a in (master_old, first_old, second_old)]
    healthy, slice_table, *arrays = (
        pltpu.with_memory_space_constraint(a, pltpu.HBM) for a in (healthy, slice_table, *arrays)
    )
    tile = arrays[0].shape[5:]
    anywhere = pl.BlockSpec(memory_space=pltpu.HBM)
    vmem = pl.BlockSpec(memory_space=pltpu.VMEM)
    dma = pltpu.SemaphoreType.DMA

    def buffer(*shape):
        return pltpu.VMEM((*shape, *tile), jnp.float32)

    def sums(*shape):
        return pltpu.VMEM((*shape, 2, 128), jnp.float32)

    out, checks = pl.pallas_call(
        functools.partial(kernel, n_inst, n_shard),
        out_shape=(
            jax.ShapeDtypeStruct((KINDS, *pieces, *tile), jnp.float32),
            jax.ShapeDtypeStruct((2, 128), jnp.float32),
        ),
        in_specs=[anywhere] * 5,
        out_specs=(vmem, vmem),
        scratch_shapes=[
            buffer(*pieces, KINDS),
            buffer(CHUNKS, 2, spots, 2, KINDS),
            buffer(CHUNKS, 2, spots, 2, KINDS),
            buffer(CHUNKS, 2, spots, KINDS),
            buffer(CHUNKS, 2, spots, KINDS),
            buffer(CHUNKS, n_shard, KINDS),
            sums(), sums(n_inst), sums(), sums(SIDE), sums(), sums(SIDE),
            pltpu.SMEM(healthy.shape, jnp.int32),
            pltpu.SMEM(slice_table.shape, jnp.int32),
            dma((KINDS + 2,)),
            dma((CHUNKS, 4)), dma((CHUNKS, 4)),
            dma((CHUNKS,)), dma((CHUNKS,)),
            dma((CHUNKS,)), dma((CHUNKS,)), dma((CHUNKS, 4)),
            dma((CHUNKS, 4)), dma((CHUNKS, 4)),
            dma, dma, dma, dma, dma, dma,
            *[buffer(3 * n_shard, KINDS) for _ in range(CHUNKS)],
        ],
        compiler_params=pltpu.CompilerParams(collective_id=0, has_side_effects=True, vmem_limit_bytes=16 << 20),
    )(healthy, slice_table, *arrays)
    state = jax.ShapeDtypeStruct((columns // 128, rows, 128), jnp.float32)
    *outs, half, checksum = pl.pallas_call(
        functools.partial(finish, 1.0 / (101.0 * 2.0 * columns)),
        out_shape=(
            state, state, state,
            jax.ShapeDtypeStruct((1, rows, columns), jnp.bfloat16),
            jax.ShapeDtypeStruct((1, 2), jnp.float32),
        ),
        in_specs=[vmem, vmem],
        out_specs=(*[pl.BlockSpec(memory_space=pltpu.HBM)] * 4, vmem),
        scratch_shapes=[pltpu.VMEM((1, rows, columns), jnp.bfloat16), dma((KINDS + 1,))],
        compiler_params=pltpu.CompilerParams(vmem_limit_bytes=4 << 20),
    )(out.reshape(KINDS, columns // 128, rows, 128), checks)
    return *(from_pieces(a, rows, columns) for a in outs), half, checksum


def solution(mesh):
    per_slice = P("inst", "shard", None)
    return jax.shard_map(
        functools.partial(on_device, mesh.shape["inst"], mesh.shape["shard"]),
        mesh=mesh,
        in_specs=(per_slice, per_slice, per_slice, P(), P()),
        out_specs=(per_slice, per_slice, per_slice, per_slice, P("inst", None)),
        check_vma=False,
    )
```

```python
import functools
import math

import jax
import jax.numpy as jnp
from jax import lax
from jax.experimental import pallas as pl
from jax.experimental.pallas import tpu as pltpu
from jax.sharding import PartitionSpec as P

MESH = pl.DeviceIdType.MESH
KINDS = 3
CHUNKS = 2
SIDE = 8


def to_pieces(shard, pieces):
    rows, columns = shard.shape[1:]
    lines = shard.reshape(rows, columns // 128, 128).transpose(1, 0, 2)
    return lines.reshape(*pieces, rows * columns // (128 * math.prod(pieces)), 128)


def from_pieces(pieces, rows, columns):
    lines = pieces.reshape(columns // 128, rows, 128)
    return lines.transpose(1, 0, 2).reshape(1, rows, columns)


def mod_101(x):
    return x - ((x * 10382) >> 20) * 101


def kernel(n_inst, n_shard, healthy_in, table_in, master, first, second, final, sums_out,
           own, cross_in, cross_out, level_in, level_out, staged,
           part, part_got, row, row_got, total, total_got,
           healthy, table, load_sem, relay_send, relay_recv, spread_send, spread_recv,
           deal_send, deal_recv, pass_recv, far_send, far_recv,
           part_send, part_recv, row_send, row_recv, total_send, total_recv, *got):
    inst = lax.axis_index("inst")
    shard = lax.axis_index("shard")
    spots = n_shard // 4
    spot, level, core = shard // 4, lax.rem(shard // 2, 2), lax.rem(shard, 2)
    flip = 1 - level
    height = own.shape[6]
    after = lax.rem(inst + 1, n_inst)
    across = lax.rem(inst + 2, n_inst)
    before = lax.rem(inst + 3, n_inst)
    near = lax.rem(inst + 3 + 2 * level, n_inst)
    far = lax.rem(inst + 1 + 2 * level, n_inst)

    def far_first(step):
        to_y = lax.rem(spot // 4 + 6 - step // 4, 4)
        to_x = lax.rem(lax.rem(spot, 4) + 6 - lax.rem(step, 4), 4)
        return to_y * 4 + to_x

    def copy(source, target, send_sem, recv_sem, to_inst, to_shard):
        return pltpu.make_async_remote_copy(
            src_ref=source,
            dst_ref=target,
            send_sem=send_sem,
            recv_sem=recv_sem,
            device_id=(to_inst, to_shard),
            device_id_type=MESH,
        )

    def waiting(target, send_sem, recv_sem):
        return copy(target, target, send_sem, recv_sem, inst, shard)

    loads = [
        pltpu.make_async_copy(source, own.at[:, :, :, :, :, kind], load_sem.at[kind])
        for kind, source in enumerate((master, first, second))
    ]
    loads += [
        pltpu.make_async_copy(healthy_in, healthy, load_sem.at[KINDS]),
        pltpu.make_async_copy(table_in, table, load_sem.at[KINDS + 1]),
    ]
    for load in loads:
        load.start()

    barrier = pltpu.get_barrier_semaphore()

    def greet(to_inst, to_shard):
        pl.semaphore_signal(barrier, inc=1, device_id=(to_inst, to_shard), device_id_type=MESH)

    def greet_spot(step, carry):
        to_y = lax.rem(spot // 4 + 6 - step // 4, 4)
        to_x = lax.rem(lax.rem(spot, 4) + 6 - lax.rem(step, 4), 4)
        to = (to_y * 4 + to_x) * 4
        for to_core in range(2):
            greet(near, to + 2 * flip + to_core)
            greet(after, to + 2 * level + to_core)
            greet(before, to + 2 * level + to_core)
            greet(inst, to + 2 * flip + to_core)

        @pl.when(to != spot * 4)
        def _():
            for to_core in range(2):
                greet(inst, to + 2 * level + to_core)

        return carry

    lax.fori_loop(0, spots, greet_spot, 0)
    greet(inst, spot * 4 + 2 * level + 1 - core)
    greet(across, shard)

    for load in loads:
        load.wait()

    shape = (1, 1, 4, 2, 2, height, 128)
    at_spot = lax.broadcasted_iota(jnp.int32, shape, 2)
    at_level = lax.broadcasted_iota(jnp.int32, shape, 3)
    at_core = lax.broadcasted_iota(jnp.int32, shape, 4)
    line = lax.broadcasted_iota(jnp.int32, shape, 5)
    lane = lax.broadcasted_iota(jnp.int32, shape, 6)
    slice_0, slice_1 = table[2 * shard], table[2 * shard + 1]
    row_base = jnp.where((line & 1) == 0, slice_0 * 88, slice_1 * 88)
    width = 64 * height
    base = row_base + (at_spot * 4 + at_level * 2 + at_core) * width + (line >> 1) * 128 + lane
    blocks = spots // 4

    def weigh(step, carry):
        all_sum, master_sum = carry
        chunk = step // (n_inst * blocks)
        of_inst = lax.rem(step // blocks, n_inst)
        at = pl.ds(lax.rem(step, blocks) * 4, 4)
        key = mod_101(mod_101(base + step * (16 * width)) * 37) + 1
        key = key.astype(jnp.float32)
        m, f, s = (own[pl.ds(chunk, 1), pl.ds(of_inst, 1), at, :, :, kind] for kind in range(KINDS))
        term = m * key
        return all_sum + (term + (f + s) * key), master_sum + term

    zero = jnp.zeros(shape, jnp.float32)
    sums = lax.fori_loop(0, CHUNKS * n_inst * blocks, weigh, (zero, zero))
    of_mine = healthy[shard]
    both = jnp.stack([s.reshape(16 * height, 128).sum(axis=0) for s in sums])
    part[...] = jnp.where(of_mine == inst, both, 0.0)

    pl.semaphore_wait(barrier, 5 * n_shard // 2)

    for to_inst in (after, across, before):
        copy(part, part_got.at[inst], part_send, part_recv, to_inst, shard).start()
    part_got[inst] = part[...]

    def relays(chunk):
        return (
            (own.at[chunk, far, :, flip], cross_in.at[chunk, 0], 0, far),
            (own.at[chunk, across, :, flip], cross_in.at[chunk, 1], 1, near),
            (own.at[chunk, across, :, level, 0], level_in.at[chunk, 0], 2, after),
            (own.at[chunk, across, :, level, 1], level_in.at[chunk, 1], 3, before),
        )

    def relay(chunk):
        for source, target, which, to_inst in relays(chunk):
            copy(source, target, relay_send.at[chunk, which], relay_recv.at[chunk, which], to_inst, shard).start()

    def spread_to(chunk, source, slot, to_inst, to_shard):
        copy(
            source, got[chunk].at[slot * n_shard + shard],
            spread_send.at[chunk], spread_recv.at[chunk], to_inst, to_shard,
        ).start()

    def spread_own(chunk):
        got[chunk][shard] = own[chunk, inst, spot, level, core]
        partner = 1 - core
        spread_to(chunk, own.at[chunk, inst, spot, level, partner], 0, inst, spot * 4 + 2 * level + partner)

        def spread(step, carry):
            to = lax.rem(spot + step, spots)
            to_shard = to * 4 + 2 * level
            spread_to(chunk, own.at[chunk, after, to, level, 1], 1, after, to_shard + 1)
            spread_to(chunk, own.at[chunk, before, to, level, 0], 2, before, to_shard)

            @pl.when(step > 0)
            def _():
                spread_to(chunk, own.at[chunk, inst, to, level, 0], 0, inst, to_shard)
                spread_to(chunk, own.at[chunk, inst, to, level, 1], 0, inst, to_shard + 1)

            return carry

        lax.fori_loop(0, spots, spread, 0)

    def mix(chunk):
        for _, target, which, _ in relays(chunk):
            waiting(target, relay_send.at[chunk, which], relay_recv.at[chunk, which]).wait_recv()

        def at_spots(step, carry):
            at = pl.ds(step * 4, 4)
            for which, from_inst, to_inst in ((0, near, inst), (1, far, near)):
                cross_out[chunk, which, at] = jnp.where(
                    of_mine == from_inst, cross_in[chunk, which, at], own[chunk, to_inst, at, flip]
                )
            for which, from_inst, to_inst in ((0, before, after), (1, after, before)):
                level_out[chunk, which, at] = jnp.where(
                    of_mine == from_inst, level_in[chunk, which, at], own[chunk, to_inst, at, level, which]
                )
            return carry

        lax.fori_loop(0, spots // 4, at_spots, 0)

    def spread_mixed(chunk):
        def spread(step, carry):
            to = far_first(step)
            for to_core in range(2):
                to_shard = to * 4 + 2 * flip + to_core
                spread_to(chunk, cross_out.at[chunk, 1, to, to_core], 2 - level, near, to_shard)
                spread_to(chunk, cross_out.at[chunk, 0, to, to_core], 0, inst, to_shard)
            to_shard = to * 4 + 2 * level
            spread_to(chunk, level_out.at[chunk, 0, to], 1, after, to_shard)
            spread_to(chunk, level_out.at[chunk, 1, to], 2, before, to_shard + 1)
            return carry

        lax.fori_loop(0, spots, spread, 0)

    relay(0)
    spread_own(0)
    for chunk in range(1, CHUNKS):
        relay(chunk)

    some = pl.ds(0, n_inst - 1)
    waiting(part_got.at[some], part_send, part_recv).wait()
    row[...] = part_got[...].sum(axis=0)
    side_at, place = shard // SIDE, lax.rem(shard, SIDE)

    def share_row(step, carry):
        to = lax.rem(place + step, SIDE)
        copy(row, row_got.at[place], row_send, row_recv, inst, side_at * SIDE + to).start()
        return carry

    lax.fori_loop(1, SIDE, share_row, 0)
    row_got[place] = row[...]

    for chunk in range(CHUNKS):
        mix(chunk)
        spread_mixed(chunk)
        if chunk + 1 < CHUNKS:
            spread_own(chunk + 1)

    rotation = table[0] >> 1
    came = pl.ds(0, 5 * n_shard // 2 - 1)

    def held(chunk, owner):
        turn = (healthy[owner] - inst) & 3
        of_level = (owner >> 1) & 1
        same = jnp.where(turn == 0, 0, jnp.where(turn == 3, 1, jnp.where(turn == 1, 2, 1 + core)))
        beside = jnp.where(of_level == 1, 1, 3)
        other = jnp.where((turn == 0) | (turn == beside), 0, 2 - of_level)
        slot = jnp.where(of_level == level, same, other)
        return got[chunk][slot * n_shard + owner]

    def deal(chunk):
        waiting(got[chunk].at[came], spread_send.at[chunk], spread_recv.at[chunk]).wait_recv()

        def stage(new, carry):
            low = held(chunk, (new - rotation - 1) & (n_shard - 1))
            high = held(chunk, (new - rotation) & (n_shard - 1))
            lines = []
            for at in range(0, height, 2):
                lines += [low[:, at + 1:at + 2], high[:, at:at + 1]]
            staged[chunk, new] = jnp.concatenate(lines, axis=1)
            return carry

        lax.fori_loop(0, n_shard, stage, 0)
        place_there = final.at[:, chunk, inst, spot, level, core]

        def deal_to(recv_sem, to_inst, to_shard):
            copy(staged.at[chunk, to_shard], place_there, deal_send.at[chunk], recv_sem, to_inst, to_shard).start()

        def deal_cross(step, carry):
            to = far_first(step) * 4 + 2 * flip
            for to_core in range(2):
                deal_to(pass_recv.at[chunk, 0], inst, to + to_core)
                deal_to(pass_recv.at[chunk, 1], near, to + to_core)
            return carry

        passing = lax.rem(inst + 3 + 2 * core, n_inst)
        resting = lax.rem(inst + 1 + 2 * core, n_inst)

        def deal_passed(step, carry):
            to = far_first(step) * 4 + 2 * level
            for to_core in range(2):
                deal_to(pass_recv.at[chunk, 2 + core], passing, to + to_core)
            return carry

        def deal_rest(step, carry):
            to = lax.rem(spot + step, spots) * 4 + 2 * level
            for to_core in range(2):
                deal_to(deal_recv.at[chunk], resting, to + to_core)

            @pl.when(step > 0)
            def _():
                for to_core in range(2):
                    deal_to(deal_recv.at[chunk], inst, to + to_core)

            return carry

        lax.fori_loop(0, spots, deal_cross, 0)
        lax.fori_loop(0, spots, deal_passed, 0)
        lax.fori_loop(0, spots, deal_rest, 0)
        deal_to(deal_recv.at[chunk], inst, spot * 4 + 2 * level + 1 - core)
        final[:, chunk, inst, spot, level, core] = staged[chunk, shard]

    def passes(chunk):
        return (
            (final.at[:, chunk, inst, :, flip], near),
            (final.at[:, chunk, near, :, flip], far),
            (final.at[:, chunk, after, :, level, 0], before),
            (final.at[:, chunk, before, :, level, 1], after),
        )

    def passed(chunk):
        return (
            final.at[:, chunk, far, :, flip],
            final.at[:, chunk, across, :, flip],
            final.at[:, chunk, across, :, level, 0],
            final.at[:, chunk, across, :, level, 1],
        )

    def pass_on(chunk):
        for which, (there, to_inst) in enumerate(passes(chunk)):
            waiting(there, deal_send.at[chunk], pass_recv.at[chunk, which]).wait_recv()
            copy(there, there, far_send.at[chunk, which], far_recv.at[chunk, which], to_inst, shard).start()

    for chunk in range(CHUNKS):
        deal(chunk)
        if chunk == 0:
            few = pl.ds(0, SIDE - 1)
            waiting(row_got.at[few], row_send, row_recv).wait()
            total[...] = row_got[...].sum(axis=0)

            def share_total(step, carry):
                to = lax.rem(side_at + step, SIDE)
                copy(total, total_got.at[side_at], total_send, total_recv, inst, to * SIDE + place).start()
                return carry

            lax.fori_loop(1, SIDE, share_total, 0)
            total_got[side_at] = total[...]
    for chunk in range(CHUNKS):
        pass_on(chunk)

    waiting(total_got.at[pl.ds(0, SIDE - 1)], total_send, total_recv).wait()
    sums_out[...] = total_got[...].sum(axis=0)

    rest = pl.ds(0, n_shard - 1)
    for chunk in range(CHUNKS):
        waiting(got[chunk].at[rest], deal_send.at[chunk], deal_recv.at[chunk]).wait_recv()
        for which, there in enumerate(passed(chunk)):
            waiting(there, far_send.at[chunk, which], far_recv.at[chunk, which]).wait_recv()
    for chunk in range(CHUNKS):
        waiting(got[chunk].at[came], spread_send.at[chunk], spread_recv.at[chunk]).wait_send()
        waiting(got[chunk].at[came], deal_send.at[chunk], deal_recv.at[chunk]).wait_send()
        for _, target, which, _ in relays(chunk):
            waiting(target, relay_send.at[chunk, which], relay_recv.at[chunk, which]).wait_send()
        for which, there in enumerate(passed(chunk)):
            waiting(there, far_send.at[chunk, which], far_recv.at[chunk, which]).wait_send()


def finish(scale, state, checks, master, first, second, half, checksum, halved, sem):
    stores = [
        pltpu.make_async_copy(state.at[kind], target, sem.at[kind])
        for kind, target in enumerate((master, first, second))
    ]
    for store in stores:
        store.start()
    tiles = state.shape[1]

    def narrow(step, carry):
        for tile in range(8):
            at = pl.ds(pl.multiple_of((step * 8 + tile) * 128, 128), 128)
            halved[0, :, at] = state[0, step * 8 + tile].astype(jnp.bfloat16)
        return carry

    lax.fori_loop(0, tiles // 8, narrow, 0, unroll=4)
    last = pltpu.make_async_copy(halved, half, sem.at[KINDS])
    last.start()
    checksum[...] = checks[...].sum(axis=1).reshape(1, 2) * scale
    for store in stores:
        store.wait()
    last.wait()


def on_device(n_inst, n_shard, master_old, first_old, second_old, healthy, slice_table):
    rows, columns = master_old.shape[1:]
    spots = n_shard // 4
    pieces = (CHUNKS, n_inst, spots, 2, 2)
    arrays = [to_pieces(a, pieces) for a in (master_old, first_old, second_old)]
    healthy, slice_table, *arrays = (
        pltpu.with_memory_space_constraint(a, pltpu.HBM) for a in (healthy, slice_table, *arrays)
    )
    tile = arrays[0].shape[5:]
    anywhere = pl.BlockSpec(memory_space=pltpu.HBM)
    vmem = pl.BlockSpec(memory_space=pltpu.VMEM)
    dma = pltpu.SemaphoreType.DMA

    def buffer(*shape):
        return pltpu.VMEM((*shape, *tile), jnp.float32)

    def sums(*shape):
        return pltpu.VMEM((*shape, 2, 128), jnp.float32)

    out, checks = pl.pallas_call(
        functools.partial(kernel, n_inst, n_shard),
        out_shape=(
            jax.ShapeDtypeStruct((KINDS, *pieces, *tile), jnp.float32),
            jax.ShapeDtypeStruct((2, 128), jnp.float32),
        ),
        in_specs=[anywhere] * 5,
        out_specs=(vmem, vmem),
        scratch_shapes=[
            buffer(*pieces, KINDS),
            buffer(CHUNKS, 2, spots, 2, KINDS),
            buffer(CHUNKS, 2, spots, 2, KINDS),
            buffer(CHUNKS, 2, spots, KINDS),
            buffer(CHUNKS, 2, spots, KINDS),
            buffer(CHUNKS, n_shard, KINDS),
            sums(), sums(n_inst), sums(), sums(SIDE), sums(), sums(SIDE),
            pltpu.SMEM(healthy.shape, jnp.int32),
            pltpu.SMEM(slice_table.shape, jnp.int32),
            dma((KINDS + 2,)),
            dma((CHUNKS, 4)), dma((CHUNKS, 4)),
            dma((CHUNKS,)), dma((CHUNKS,)),
            dma((CHUNKS,)), dma((CHUNKS,)), dma((CHUNKS, 4)),
            dma((CHUNKS, 4)), dma((CHUNKS, 4)),
            dma, dma, dma, dma, dma, dma,
            *[buffer(3 * n_shard, KINDS) for _ in range(CHUNKS)],
        ],
        compiler_params=pltpu.CompilerParams(collective_id=0, has_side_effects=True, vmem_limit_bytes=16 << 20),
    )(healthy, slice_table, *arrays)
    state = jax.ShapeDtypeStruct((columns // 128, rows, 128), jnp.float32)
    *outs, half, checksum = pl.pallas_call(
        functools.partial(finish, 1.0 / (101.0 * 2.0 * columns)),
        out_shape=(
            state, state, state,
            jax.ShapeDtypeStruct((1, rows, columns), jnp.bfloat16),
            jax.ShapeDtypeStruct((1, 2), jnp.float32),
        ),
        in_specs=[vmem, vmem],
        out_specs=(*[pl.BlockSpec(memory_space=pltpu.HBM)] * 4, vmem),
        scratch_shapes=[pltpu.VMEM((1, rows, columns), jnp.bfloat16), dma((KINDS + 1,))],
        compiler_params=pltpu.CompilerParams(vmem_limit_bytes=4 << 20),
    )(out.reshape(KINDS, columns // 128, rows, 128), checks)
    return *(from_pieces(a, rows, columns) for a in outs), half, checksum


def solution(mesh):
    per_slice = P("inst", "shard", None)
    return jax.shard_map(
        functools.partial(on_device, mesh.shape["inst"], mesh.shape["shard"]),
        mesh=mesh,
        in_specs=(per_slice, per_slice, per_slice, P(), P()),
        out_specs=(per_slice, per_slice, per_slice, per_slice, P("inst", None)),
        check_vma=False,
    )
```
